32 devices in a mesh: row: 4 (over z), col: 8 (over y, x, core).
Axes of the slice: x: 2, y: 2, z: 4, core: 2. Of those that a mesh axis runs over, the one named last changes fastest.
Arguments:
- tile_data: bfloat16 [8, 4, 8, 2, 128, 128], P(None, 'row', 'col'), may hold values from 0 to 1, as said below
- tile_cols: int32 [8, 4, 8, 2], P(None, 'row', 'col'), may hold values from -1 to 31, as said below
Outputs:
- vertex_triangles: float32 [8, 4, 128], P(None, 'row', 'col')
- triangles: float32 [], replicated
The draws below stay inside these ranges and needn't reach their ends.
Inputs may be any that keep to these rules, and one draw needn't show every extreme that they name: `tile_cols`: slot (a, r, c, s) holds -1 (empty) or a tile column J with J % 8 == c and J >= a 4 + r; the columns of one tile row are distinct; every slot of tile row 0 is filled; tile row I keeps each slot that has an allowed column with probability (32 - I) / 32, so rows with a lower index hold more tiles on average. `tile_data`: entries are 0 or 1; tiles of empty slots are zero; a tile whose column equals its tile row is strictly upper triangular; about one entry in 8 of a stored tile is 1, with edges clustered among groups of vertices.
All inputs are finite; a program needn't handle non-finite values.
Results may differ from the reference program's by a relative error of at most 0.0003.
Values may be sent and summed in bfloat16 or wider, within the bound.
A program may use at most 128 MiB of HBM per device.

```python
import jax
import jax.numpy as jnp
from jax import lax

TILE = 128
SLOT = 2
ROWS_DEV = 8
VERTICES = 4096
N_ROW = 4
N_COL = 8


def tile_structure(key):
    tile_rows = ROWS_DEV * N_ROW
    choices_per = tile_rows // N_COL
    row_ids = jnp.arange(ROWS_DEV, dtype=jnp.int32)[:, None] * N_ROW + jnp.arange(N_ROW, dtype=jnp.int32)[None, :]
    offsets = jnp.arange(choices_per, dtype=jnp.int32)
    columns = jnp.arange(N_COL, dtype=jnp.int32)[:, None] + N_COL * offsets[None, :]
    allowed = columns[None, None, :, :] >= row_ids[:, :, None, None]
    base = jax.random.fold_in(key, 11)
    first = jax.random.fold_in(base, 1)
    second = jax.random.fold_in(base, 2)
    raw = jax.random.randint(first, (ROWS_DEV, N_ROW, N_COL, choices_per), 0, 1 << 20)
    scores = jnp.where(allowed, raw * choices_per + offsets + choices_per, -1 - offsets)
    best, picked = lax.top_k(scores, SLOT)
    usable = best >= choices_per
    chance = jax.random.randint(second, (ROWS_DEV, N_ROW, N_COL, SLOT), 0, tile_rows)
    present = usable & (chance >= row_ids[:, :, None, None])
    chosen = jnp.arange(N_COL, dtype=jnp.int32)[None, None, :, None] + N_COL * picked.astype(jnp.int32)
    return jnp.where(present, chosen, -1).astype(jnp.int32)


def draw_tile_cols(key, part):
    return tile_structure(key)


def draw_tile_data(key, part):
    tile_rows = ROWS_DEV * N_ROW
    columns = tile_structure(key)
    row_ids = jnp.arange(ROWS_DEV, dtype=jnp.int32)[:, None] * N_ROW + jnp.arange(N_ROW, dtype=jnp.int32)[None, :]
    labels = jax.random.randint(jax.random.fold_in(key, 31), (tile_rows, TILE), 0, 4).astype(jnp.int32)
    row_labels = labels[row_ids]
    clipped = jnp.clip(columns, 0, tile_rows - 1).astype(jnp.int32)
    col_labels = labels[clipped]
    same = row_labels[:, :, None, None, :, None] == col_labels[:, :, :, :, None, :]
    bits = jax.random.randint(jax.random.fold_in(key, 23), (ROWS_DEV, N_ROW, N_COL, SLOT, TILE, TILE), 0, 24)
    linked = jnp.where(same, bits < 9, bits < 1)
    upper = jnp.arange(TILE)[None, :] > jnp.arange(TILE)[:, None]
    diagonal = columns == row_ids[:, :, None, None]
    keep = (columns >= 0)[..., None, None] & ((~diagonal)[..., None, None] | upper[None, None, None, None, :, :])
    values = jnp.where(keep & linked, 1.0, 0.0).astype(jnp.float32)
    return values.astype(jnp.bfloat16)


def setup_inputs(seed: int = 0) -> dict:
    key_list = jax.random.split(jax.random.key(seed), 3)
    tile_data = draw_tile_data(jax.random.fold_in(key_list[2], 71), 0)
    tile_cols = draw_tile_cols(jax.random.fold_in(key_list[2], 71), 0)
    return dict(tile_data=tile_data, tile_cols=tile_cols)


vertex_scale = 2.0 ** -14
total_scale = 2.0 ** -12


def reference(tile_data, tile_cols):
    tile_rows = ROWS_DEV * N_ROW
    width = N_COL * SLOT
    stored = tile_data.astype(jnp.float32).reshape(tile_rows, N_COL, SLOT, TILE, TILE)
    columns = tile_cols.reshape(tile_rows, N_COL, SLOT)

    def one_row(index):
        left_tiles = stored[index].reshape(width, TILE, TILE)
        middle = columns[index].reshape(width)
        clipped = jnp.clip(middle, 0, tile_rows - 1).astype(jnp.int32)
        partner = stored[clipped]
        partner_cols = columns[clipped]
        own_cols = columns[index]
        own_tiles = stored[index]
        matches = (partner_cols[:, :, :, None] == own_cols[None, :, None, :])
        matches = matches & (middle >= 0)[:, None, None, None] & (own_cols >= 0)[None, :, None, :]
        targets = jnp.einsum("pcqs,csxz->pcqxz", matches.astype(jnp.float32), own_tiles, precision=lax.Precision.HIGHEST)
        paths = jnp.einsum("pxy,pcqyz->pcqxz", left_tiles, partner, precision=lax.Precision.HIGHEST)
        return jnp.sum(paths * targets, axis=(0, 1, 2, 4))

    counts = lax.map(one_row, jnp.arange(tile_rows, dtype=jnp.int32))
    vertex_triangles = (counts * vertex_scale).reshape(ROWS_DEV, N_ROW, TILE)
    triangles = jnp.sum(counts) * (total_scale / VERTICES)
    return vertex_triangles, triangles
```

```python
import functools
import math

import jax
import jax.numpy as jnp
from jax import lax
from jax.experimental import pallas as pl
from jax.experimental.pallas import tpu as pltpu
from jax.sharding import PartitionSpec as P

MESH = pl.DeviceIdType.MESH
vertex_scale = 2.0 ** (-14)
total_scale = 2.0 ** (-12)


def plane_shape(n_col):
    chips = n_col // 2
    side = math.isqrt(chips)
    return (side, side) if side * side == chips else (1, chips)


def kernel(n_row, n_col, tiles, cols_ref, plane_ref, total_ref,
           row_buf, col_buf, row_idx, col_idx, row_smem, col_smem, acc, parts, planes,
           load_sem, smem_sem, row_send, row_recv, col_send, col_recv,
           idx_send, idx_recv, part_send, part_recv, plane_send, plane_recv):
    r = lax.axis_index("row")
    c = lax.axis_index("col")
    n_tiles = tiles.shape[0]
    half = n_tiles // 2
    rows = acc.shape[0]
    slots = n_tiles // rows
    width = tiles.shape[1]
    zero = n_col * n_tiles
    Y, X = plane_shape(n_col)
    u = c % 2
    x = (c // 2) % X
    y = c // (2 * X)

    def col_of(yy, xx, uu):
        return (yy * X + xx) * 2 + uu

    def row_block(cc, h):
        return row_buf.at[pl.ds(cc * n_tiles + h * half, half)]

    def col_block(rr):
        return col_buf.at[pl.ds(rr * n_tiles, n_tiles)]

    load_row = pltpu.make_async_copy(tiles, row_buf.at[pl.ds(c * n_tiles, n_tiles)], load_sem.at[0])
    load_row.start()
    load_col = pltpu.make_async_copy(tiles, col_block(r), load_sem.at[1])
    load_col.start()
    load_ri = pltpu.make_async_copy(cols_ref, row_idx.at[c], load_sem.at[2])
    load_ri.start()
    load_ci = pltpu.make_async_copy(cols_ref, col_idx.at[r], load_sem.at[3])
    load_ci.start()

    barrier = pltpu.get_barrier_semaphore()
    for t in range(1, n_col):
        pl.semaphore_signal(barrier, inc=1, device_id={"col": lax.rem(c + t, n_col)}, device_id_type=MESH)
    for t in range(1, n_row):
        pl.semaphore_signal(barrier, inc=1, device_id={"row": lax.rem(r + t, n_row)}, device_id_type=MESH)
    row_buf[zero] = jnp.zeros(row_buf.shape[1:], row_buf.dtype)
    acc[...] = jnp.zeros_like(acc)
    load_row.wait()
    load_col.wait()
    pl.semaphore_wait(barrier, n_col + n_row - 2)

    sends = []

    def send_row(cc, h, dest):
        copy = pltpu.make_async_remote_copy(
            src_ref=row_block(cc, h), dst_ref=row_block(cc, h),
            send_sem=row_send.at[len(sends)], recv_sem=row_recv.at[cc, h],
            device_id={"col": dest}, device_id_type=MESH)
        copy.start()
        sends.append(copy)

    def got_row(cc, h):
        pltpu.make_async_remote_copy(
            src_ref=row_block(cc, h), dst_ref=row_block(cc, h),
            send_sem=row_send.at[0], recv_sem=row_recv.at[cc, h],
            device_id={"col": lax.rem(c + 1, n_col)}, device_id_type=MESH).wait_recv()

    def col_copy(rr, way, dest):
        return pltpu.make_async_remote_copy(
            src_ref=col_block(rr), dst_ref=col_block(rr),
            send_sem=col_send.at[rr, way], recv_sem=col_recv.at[rr],
            device_id={"row": dest}, device_id_type=MESH)

    def other(value, t, n):
        return lax.rem(value + t, n)

    def pass_on(t):
        up, down = r - t, r + t
        if t > 0:
            @pl.when(up >= 0)
            def _():
                col_copy(up, 0, r).wait_recv()
        @pl.when((up >= 0) & (r < n_row - 1))
        def _():
            col_copy(up, 0, r + 1).start()
        if t > 0:
            @pl.when(down < n_row)
            def _():
                col_copy(down, 1, r).wait_recv()
        @pl.when((down < n_row) & (r > 0))
        def _():
            col_copy(down, 1, r - 1).start()

    pass_on(0)
    xs = [col_of(y, other(x, t, X), u) for t in range(1, X)]
    ys = [col_of(other(y, t, Y), x, u) for t in range(1, Y)]
    for dest in xs:
        send_row(c, 0, dest)
    for dest in ys:
        send_row(c, 1, dest)
    load_ri.wait()
    load_ci.wait()
    idx_copies = []
    for t in range(1, n_col):
        idx_copies.append(pltpu.make_async_remote_copy(
            src_ref=row_idx.at[c], dst_ref=row_idx.at[c],
            send_sem=idx_send.at[t - 1], recv_sem=idx_recv.at[t - 1],
            device_id={"col": other(c, t, n_col)}, device_id_type=MESH))
    for t in range(1, n_row):
        idx_copies.append(pltpu.make_async_remote_copy(
            src_ref=col_idx.at[r], dst_ref=col_idx.at[r],
            send_sem=idx_send.at[n_col - 2 + t], recv_sem=idx_recv.at[n_col - 2 + t],
            device_id={"row": other(r, t, n_row)}, device_id_type=MESH))
    for copy in idx_copies:
        copy.start()
    for dest in ys:
        send_row(c, 0, dest)
    for dest in xs:
        send_row(c, 1, dest)
    for h in range(2):
        send_row(c, h, c + 1 - 2 * u)
    for t in range(1, max(X, Y)):
        if t < X:
            cc = col_of(y, other(x, t, X), u)
            got_row(cc, 0)
            for dest in ys:
                send_row(cc, 0, dest)
        if t < Y:
            cc = col_of(other(y, t, Y), x, u)
            got_row(cc, 1)
            for dest in xs:
                send_row(cc, 1, dest)
    for t in range(1, X):
        send_row(col_of(y, other(x, t, X), u), 0, c + 1 - 2 * u)
    for t in range(1, Y):
        send_row(col_of(other(y, t, Y), x, u), 1, c + 1 - 2 * u)
    if n_row > 1:
        pass_on(1)
    for t in range(1, X):
        cc = col_of(y, other(x, t, X), u)
        got_row(cc, 1)
        send_row(cc, 1, c + 1 - 2 * u)
    for t in range(1, Y):
        cc = col_of(other(y, t, Y), x, u)
        got_row(cc, 0)
        send_row(cc, 0, c + 1 - 2 * u)
    for tx in range(1, X):
        for ty in range(1, Y):
            cc = col_of(other(y, ty, Y), other(x, tx, X), u)
            for h in range(2):
                got_row(cc, h)
                send_row(cc, h, c + 1 - 2 * u)
    for m in range(n_col // 2):
        for h in range(2):
            got_row(2 * m + 1 - u, h)
    for copy in idx_copies:
        copy.wait()
    to_smem = [pltpu.make_async_copy(row_idx, row_smem, smem_sem.at[0]),
               pltpu.make_async_copy(col_idx, col_smem, smem_sem.at[1])]
    for copy in to_smem:
        copy.start()
    for copy in to_smem:
        copy.wait()

    def unit(rr):
        def step(b, carry):
            middle = b * n_row + rr
            block = lax.rem(middle, n_col)
            left = []
            for a in range(rows):
                index = jnp.int32(zero)
                for s in range(slots):
                    index = jnp.where(row_smem[block, a, s] == middle, block * n_tiles + a * slots + s, index)
                left.append(row_buf[index])
            left = jnp.concatenate(left, axis=0)
            right = jnp.concatenate(
                [col_buf[rr * n_tiles + b * slots + s] for s in range(slots)], axis=1)
            paths = jnp.dot(left, right, preferred_element_type=jnp.float32)
            for a in range(rows):
                value = acc[a]
                for s in range(slots):
                    target = col_smem[rr, b, s]
                    index = jnp.int32(zero)
                    for q in range(slots):
                        own = row_smem[c, a, q]
                        index = jnp.where((own == target) & (target >= 0), c * n_tiles + a * slots + q, index)
                    value = value + paths[a * width:(a + 1) * width, s * width:(s + 1) * width] * (
                        row_buf[index].astype(jnp.float32))
                acc[a] = value
            return carry
        lax.fori_loop(0, rows, step, 0)

    def units(t):
        @pl.when(r - t >= 0)
        def _():
            unit(r - t)
        @pl.when(r + t < n_row)
        def _():
            unit(r + t)

    for t in range(2, n_row - 1):
        pass_on(t)
    unit(r)
    for t in range(1, n_row - 1):
        units(t)
    if n_row > 2:
        pass_on(n_row - 1)
    if n_row > 1:
        units(n_row - 1)

    parts[c] = jnp.sum(acc[...], axis=2)
    out_copies = []
    for t in range(1, n_col):
        out_copies.append(pltpu.make_async_remote_copy(
            src_ref=parts.at[c], dst_ref=parts.at[c],
            send_sem=part_send.at[t - 1], recv_sem=part_recv.at[t - 1],
            device_id={"col": other(c, t, n_col)}, device_id_type=MESH))
    for copy in out_copies:
        copy.start()
    for copy in sends:
        copy.wait_send()
    for t in range(n_row):
        @pl.when((r - t >= 0) & (r < n_row - 1))
        def _():
            col_copy(r - t, 0, r).wait_send()
        @pl.when((r + t < n_row) & (r > 0))
        def _():
            col_copy(r + t, 1, r).wait_send()
    for copy in out_copies:
        copy.wait()
    plane = jnp.sum(parts[...], axis=0)
    plane_ref[...] = plane
    planes[r] = plane
    plane_copies = []
    for t in range(1, n_row):
        plane_copies.append(pltpu.make_async_remote_copy(
            src_ref=planes.at[r], dst_ref=planes.at[r],
            send_sem=plane_send.at[t - 1], recv_sem=plane_recv.at[t - 1],
            device_id={"row": other(r, t, n_row)}, device_id_type=MESH))
    for copy in plane_copies:
        copy.start()
    for copy in plane_copies:
        copy.wait()
    total_ref[...] = jnp.full(total_ref.shape, jnp.sum(planes[...]), jnp.float32)


def on_device(n_row, n_col, tile_data, tile_cols):
    rows = tile_data.shape[0]
    slots = tile_data.shape[3]
    width = tile_data.shape[4]
    n_tiles = rows * slots
    tiles = tile_data.reshape(n_tiles, width, width)
    cols = jnp.pad(tile_cols.reshape(rows, slots), ((0, 0), (0, 128 - slots)), constant_values=-1)
    Y, X = plane_shape(n_col)
    n_sends = 2 * (n_col + (X - 1) + (Y - 1)) + (X - 1) * (Y - 1) * 2 + (X - 1) + (Y - 1) + 8
    dma = pltpu.SemaphoreType.DMA
    plane, total = pl.pallas_call(
        functools.partial(kernel, n_row, n_col),
        out_shape=(jax.ShapeDtypeStruct((rows, width), jnp.float32),
                   jax.ShapeDtypeStruct((8, 128), jnp.float32)),
        in_specs=[pl.BlockSpec(memory_space=pl.ANY), pl.BlockSpec(memory_space=pl.ANY)],
        out_specs=(pl.BlockSpec(memory_space=pltpu.VMEM), pl.BlockSpec(memory_space=pltpu.VMEM)),
        scratch_shapes=[
            pltpu.VMEM((n_col * n_tiles + 1, width, width), jnp.bfloat16),
            pltpu.VMEM((n_row * n_tiles, width, width), jnp.bfloat16),
            pltpu.VMEM((n_col, rows, 128), jnp.int32),
            pltpu.VMEM((n_row, rows, 128), jnp.int32),
            pltpu.SMEM((n_col, rows, 128), jnp.int32),
            pltpu.SMEM((n_row, rows, 128), jnp.int32),
            pltpu.VMEM((rows, width, width), jnp.float32),
            pltpu.VMEM((n_col, rows, width), jnp.float32),
            pltpu.VMEM((n_row, rows, width), jnp.float32),
            dma((4,)), dma((2,)),
            dma((n_sends,)), dma((n_col, 2)),
            dma((n_row, 2)), dma((n_row,)),
            dma((n_col + n_row - 2,)), dma((n_col + n_row - 2,)),
            dma((n_col - 1,)), dma((n_col - 1,)),
            dma((max(n_row - 1, 1),)), dma((max(n_row - 1, 1),)),
        ],
        compiler_params=pltpu.CompilerParams(collective_id=0, has_side_effects=True),
    )(tiles, cols)
    share = width // n_col
    start = lax.axis_index("col") * share
    shares = lax.dynamic_slice_in_dim(plane, start, share, 1).reshape(rows, 1, share)
    vertices = rows * n_row * width
    return shares * vertex_scale, total[0, 0] * (total_scale / vertices)


def solution(mesh):
    return jax.shard_map(
        functools.partial(on_device, mesh.shape["row"], mesh.shape["col"]),
        mesh=mesh,
        in_specs=(P(None, "row", "col", None, None, None), P(None, "row", "col", None)),
        out_specs=(P(None, "row", "col"), P()),
        check_vma=False,
    )
```

```python
import functools
import math

import jax
import jax.numpy as jnp
from jax import lax
from jax.experimental import pallas as pl
from jax.experimental.pallas import tpu as pltpu
from jax.sharding import PartitionSpec as P

MESH = pl.DeviceIdType.MESH
vertex_scale = 2.0 ** (-14)
total_scale = 2.0 ** (-12)


def plane_shape(n_col):
    chips = n_col // 2
    side = math.isqrt(chips)
    return (side, side) if side * side == chips else (1, chips)


def kernel(n_row, n_col, tiles, cols_ref, plane_ref, total_ref,
           row_buf, col_buf, far_buf, row_idx, col_idx, far_idx, row_smem, col_smem, far_smem,
           acc, far_acc, parts, planes,
           load_sem, smem_sem, row_send, row_recv, col_send, col_recv,
           idx_send, idx_recv, part_send, part_recv, plane_send, plane_recv,
           far_send, far_recv, fidx_send, fidx_recv, fpart_send, fpart_recv):
    r = lax.axis_index("row")
    c = lax.axis_index("col")
    n_tiles = tiles.shape[0]
    half = n_tiles // 2
    rows = acc.shape[0]
    slots = n_tiles // rows
    width = tiles.shape[1]
    zero = n_col * n_tiles
    moved = n_row >= 4 and n_col % n_row == 0
    reach = n_row - 2 if moved else n_row - 1
    n_far = max(n_col // n_row, 1)
    far_zero = n_far * n_tiles
    low = r < n_row // 2
    inner = (r == 1) | (r == n_row - 2)
    outer = (r == 0) | (r == n_row - 1)
    far_left = jnp.where(low, 0, n_row - 1)
    far_middle = n_row - 1 - far_left
    neighbour = jnp.where(low, 1 - r, 2 * n_row - 3 - r)
    Y, X = plane_shape(n_col)
    u = c % 2
    x = (c // 2) % X
    y = c // (2 * X)

    def col_of(yy, xx, uu):
        return (yy * X + xx) * 2 + uu

    def row_block(cc, h):
        return row_buf.at[pl.ds(cc * n_tiles + h * half, half)]

    def col_block(rr):
        return col_buf.at[pl.ds(rr * n_tiles, n_tiles)]

    load_row = pltpu.make_async_copy(tiles, row_buf.at[pl.ds(c * n_tiles, n_tiles)], load_sem.at[0])
    load_row.start()
    load_col = pltpu.make_async_copy(tiles, col_block(r), load_sem.at[1])
    load_col.start()
    load_ri = pltpu.make_async_copy(cols_ref, row_idx.at[c], load_sem.at[2])
    load_ri.start()
    load_ci = pltpu.make_async_copy(cols_ref, col_idx.at[r], load_sem.at[3])
    load_ci.start()

    barrier = pltpu.get_barrier_semaphore()
    for t in range(1, n_col):
        pl.semaphore_signal(barrier, inc=1, device_id={"col": lax.rem(c + t, n_col)}, device_id_type=MESH)
    for t in range(1, n_row):
        pl.semaphore_signal(barrier, inc=1, device_id={"row": lax.rem(r + t, n_row)}, device_id_type=MESH)
    if moved:
        @pl.when(inner | outer)
        def _():
            for t in range(1, n_col):
                pl.semaphore_signal(
                    barrier, inc=1, device_id={"row": neighbour, "col": lax.rem(c + t, n_col)},
                    device_id_type=MESH)
    row_buf[zero] = jnp.zeros(row_buf.shape[1:], row_buf.dtype)
    far_buf[far_zero] = jnp.zeros(far_buf.shape[1:], far_buf.dtype)
    col_buf[n_row * n_tiles] = jnp.zeros(col_buf.shape[1:], col_buf.dtype)
    acc[...] = jnp.zeros_like(acc)
    far_acc[...] = jnp.zeros_like(far_acc)
    load_row.wait()
    load_col.wait()
    greeted = jnp.where(inner | outer, n_col - 1, 0) if moved else 0
    pl.semaphore_wait(barrier, n_col + n_row - 2 + greeted)

    sends = []

    def send_row(cc, h, dest):
        copy = pltpu.make_async_remote_copy(
            src_ref=row_block(cc, h), dst_ref=row_block(cc, h),
            send_sem=row_send.at[len(sends)], recv_sem=row_recv.at[cc, h],
            device_id={"col": dest}, device_id_type=MESH)
        copy.start()
        sends.append(copy)

    def got_row(cc, h):
        pltpu.make_async_remote_copy(
            src_ref=row_block(cc, h), dst_ref=row_block(cc, h),
            send_sem=row_send.at[0], recv_sem=row_recv.at[cc, h],
            device_id={"col": lax.rem(c + 1, n_col)}, device_id_type=MESH).wait_recv()

    def col_copy(rr, way, dest):
        return pltpu.make_async_remote_copy(
            src_ref=col_block(rr), dst_ref=col_block(rr),
            send_sem=col_send.at[rr, way], recv_sem=col_recv.at[rr],
            device_id={"row": dest}, device_id_type=MESH)

    def other(value, t, n):
        return lax.rem(value + t, n)

    def pass_on(t):
        up, down = r - t, r + t
        if t > 0:
            @pl.when(up >= 0)
            def _():
                col_copy(up, 0, r).wait_recv()
        if t < reach:
            @pl.when((up >= 0) & (r < n_row - 1))
            def _():
                col_copy(up, 0, r + 1).start()
        if t > 0:
            @pl.when(down < n_row)
            def _():
                col_copy(down, 1, r).wait_recv()
        if t < reach:
            @pl.when((down < n_row) & (r > 0))
            def _():
                col_copy(down, 1, r - 1).start()

    pass_on(0)
    xs = [col_of(y, other(x, t, X), u) for t in range(1, X)]
    ys = [col_of(other(y, t, Y), x, u) for t in range(1, Y)]
    for dest in xs:
        send_row(c, 0, dest)
    for dest in ys:
        send_row(c, 1, dest)
    load_ri.wait()
    load_ci.wait()
    idx_copies = []
    for t in range(1, n_col):
        idx_copies.append(pltpu.make_async_remote_copy(
            src_ref=row_idx.at[c], dst_ref=row_idx.at[c],
            send_sem=idx_send.at[t - 1], recv_sem=idx_recv.at[t - 1],
            device_id={"col": other(c, t, n_col)}, device_id_type=MESH))
    for t in range(1, n_row):
        idx_copies.append(pltpu.make_async_remote_copy(
            src_ref=col_idx.at[r], dst_ref=col_idx.at[r],
            send_sem=idx_send.at[n_col - 2 + t], recv_sem=idx_recv.at[n_col - 2 + t],
            device_id={"row": other(r, t, n_row)}, device_id_type=MESH))
    for copy in idx_copies:
        copy.start()
    for dest in ys:
        send_row(c, 0, dest)
    for dest in xs:
        send_row(c, 1, dest)
    for h in range(2):
        send_row(c, h, c + 1 - 2 * u)
    for t in range(1, max(X, Y)):
        if t < X:
            cc = col_of(y, other(x, t, X), u)
            got_row(cc, 0)
            for dest in ys:
                send_row(cc, 0, dest)
        if t < Y:
            cc = col_of(other(y, t, Y), x, u)
            got_row(cc, 1)
            for dest in xs:
                send_row(cc, 1, dest)
    for t in range(1, X):
        send_row(col_of(y, other(x, t, X), u), 0, c + 1 - 2 * u)
    for t in range(1, Y):
        send_row(col_of(other(y, t, Y), x, u), 1, c + 1 - 2 * u)
    if n_row > 1:
        pass_on(1)

    ways = X + Y

    def far_block(e, h):
        return far_buf.at[pl.ds(e * n_tiles + h * half, half)]

    def far_copy(e, h, way, dest, source=None):
        return pltpu.make_async_remote_copy(
            src_ref=far_block(e, h) if source is None else source, dst_ref=far_block(e, h),
            send_sem=far_send.at[e, h, way], recv_sem=far_recv.at[e, h],
            device_id={"col": dest}, device_id_type=MESH)

    def far_index(e, t):
        return pltpu.make_async_remote_copy(
            src_ref=far_idx.at[e], dst_ref=far_idx.at[e],
            send_sem=fidx_send.at[e, t - 1], recv_sem=fidx_recv.at[e],
            device_id={"col": other(c, t, n_col)}, device_id_type=MESH)

    def far_tiles(e):
        return pltpu.make_async_copy(
            col_buf.at[pl.ds(far_left * n_tiles, n_tiles)],
            far_buf.at[pl.ds(e * n_tiles, n_tiles)], load_sem.at[4])

    def far_place(e):
        cc = e * n_row + far_middle
        return cc, (cc % 2) == u, ((cc // 2) % X) == x, (cc // (2 * X)) == y

    partner = c + 1 - 2 * u
    to_x = [(t, dest) for t, dest in enumerate(xs, 1)]
    to_y = [(X - 1 + t, dest) for t, dest in enumerate(ys, 1)]

    def far_source():
        for e in range(n_far):
            cc, same_u, same_x, same_y = far_place(e)

            @pl.when(inner & (cc == c))
            def _():
                source = col_buf.at[pl.ds(far_left * n_tiles, half)]
                source2 = col_buf.at[pl.ds(far_left * n_tiles + half, half)]
                for way, dest in to_x:
                    far_copy(e, 0, way, dest, source).start()
                for way, dest in to_y:
                    far_copy(e, 1, way, dest, source2).start()
                for way, dest in to_y:
                    far_copy(e, 0, way, dest, source).start()
                for way, dest in to_x:
                    far_copy(e, 1, way, dest, source2).start()
                far_copy(e, 0, 0, partner, source).start()
                far_copy(e, 1, 0, partner, source2).start()
                far_tiles(e).start()
                index = pltpu.make_async_copy(col_idx.at[far_left], far_idx.at[e], load_sem.at[5])
                index.start()
                index.wait()
                for t in range(1, n_col):
                    far_index(e, t).start()

    def far_relay(first):
        for e in range(n_far):
            cc, same_u, same_x, same_y = far_place(e)
            here = inner & same_u & (cc != c)

            @pl.when(here & same_y)
            def _():
                h = 0 if first else 1
                far_copy(e, h, 0, partner).wait_recv()
                if first:
                    for way, dest in to_y:
                        far_copy(e, 0, way, dest).start()
                far_copy(e, h, 0, partner).start()

            @pl.when(here & same_x)
            def _():
                h = 1 if first else 0
                far_copy(e, h, 0, partner).wait_recv()
                if first:
                    for way, dest in to_x:
                        far_copy(e, 1, way, dest).start()
                far_copy(e, h, 0, partner).start()

            if not first:
                @pl.when(here & jnp.logical_not(same_x | same_y))
                def _():
                    for h in range(2):
                        far_copy(e, h, 0, partner).wait_recv()
                        far_copy(e, h, 0, partner).start()

    def far_end():
        for e in range(n_far):
            cc, same_u, same_x, same_y = far_place(e)

            @pl.when(inner & jnp.logical_not(same_u))
            def _():
                for h in range(2):
                    far_copy(e, h, 0, partner).wait_recv()

            @pl.when(inner & (cc != c))
            def _():
                far_index(e, 1).wait_recv()

            @pl.when(inner & (cc == c))
            def _():
                far_tiles(e).wait()
                for t in range(1, n_col):
                    far_index(e, t).wait_send()
                for h in range(2):
                    for way in range(ways - 1):
                        far_copy(e, h, way, partner).wait_send()

            @pl.when(inner & same_u & (cc != c))
            def _():
                for h in range(2):
                    far_copy(e, h, 0, partner).wait_send()

            @pl.when(inner & same_u & (cc != c) & same_y)
            def _():
                for way, dest in to_y:
                    far_copy(e, 0, way, dest).wait_send()

            @pl.when(inner & same_u & (cc != c) & same_x)
            def _():
                for way, dest in to_x:
                    far_copy(e, 1, way, dest).wait_send()

    for copy in idx_copies:
        copy.wait()
    if moved:
        far_source()
    for t in range(1, X):
        cc = col_of(y, other(x, t, X), u)
        got_row(cc, 1)
        send_row(cc, 1, c + 1 - 2 * u)
    for t in range(1, Y):
        cc = col_of(other(y, t, Y), x, u)
        got_row(cc, 0)
        send_row(cc, 0, c + 1 - 2 * u)
    for tx in range(1, X):
        for ty in range(1, Y):
            cc = col_of(other(y, ty, Y), other(x, tx, X), u)
            for h in range(2):
                got_row(cc, h)
                send_row(cc, h, c + 1 - 2 * u)
    for m in range(n_col // 2):
        for h in range(2):
            got_row(2 * m + 1 - u, h)
    to_smem = [pltpu.make_async_copy(row_idx, row_smem, smem_sem.at[0]),
               pltpu.make_async_copy(col_idx, col_smem, smem_sem.at[1])]
    for copy in to_smem:
        copy.start()
    for copy in to_smem:
        copy.wait()

    def unit(rr, left_slot, left_buf, left_zero, own_slot, own_buf, own_zero, own_base, total):
        def step(b, carry):
            middle = b * n_row + rr
            block = lax.rem(middle, n_col)
            left = []
            for a in range(rows):
                index = jnp.int32(left_zero)
                for s in range(slots):
                    held, base = left_slot(block, a, s)
                    index = jnp.where(held == middle, base + a * slots + s, index)
                left.append(left_buf[index])
            left = jnp.concatenate(left, axis=0)
            right = jnp.concatenate(
                [col_buf[rr * n_tiles + b * slots + s] for s in range(slots)], axis=1)
            paths = jnp.dot(left, right, preferred_element_type=jnp.float32)
            for a in range(rows):
                value = total[a]
                for s in range(slots):
                    target = col_smem[rr, b, s]
                    index = jnp.int32(own_zero)
                    for q in range(slots):
                        own = own_slot(a, q)
                        index = jnp.where((own == target) & (target >= 0), own_base + a * slots + q, index)
                    value = value + paths[a * width:(a + 1) * width, s * width:(s + 1) * width] * (
                        own_buf[index].astype(jnp.float32))
                total[a] = value
            return carry
        lax.fori_loop(0, rows, step, 0)

    def near_unit(rr):
        unit(rr, lambda block, a, s: (row_smem[block, a, s], block * n_tiles), row_buf, zero,
             lambda a, q: row_smem[c, a, q], row_buf, zero, c * n_tiles, acc)

    def far_unit():
        unit(far_middle,
             lambda block, a, s: (far_smem[block // n_row, a, s], (block // n_row) * n_tiles),
             far_buf, far_zero,
             lambda a, q: col_smem[far_left, a, q], col_buf, n_row * n_tiles,
             far_left * n_tiles, far_acc)

    def units(t):
        @pl.when(r - t >= 0)
        def _():
            near_unit(r - t)
        @pl.when(r + t < n_row)
        def _():
            near_unit(r + t)

    for t in range(2, reach):
        pass_on(t)
    if moved:
        far_relay(True)
    near_unit(r)
    for t in range(1, reach):
        units(t)
    if moved:
        far_relay(False)
    if reach > 1:
        pass_on(reach)
    if reach > 0:
        units(reach)
    if moved:
        far_end()

        @pl.when(inner)
        def _():
            copy = pltpu.make_async_copy(far_idx, far_smem, smem_sem.at[2])
            copy.start()
            copy.wait()
            far_unit()
            parts[n_col + c] = jnp.sum(far_acc[...], axis=2)

    def far_part(t):
        return pltpu.make_async_remote_copy(
            src_ref=parts.at[n_col + c], dst_ref=parts.at[n_col + c],
            send_sem=fpart_send.at[t], recv_sem=fpart_recv.at[t],
            device_id={"row": neighbour, "col": other(c, t, n_col)}, device_id_type=MESH)

    if moved:
        @pl.when(inner)
        def _():
            for t in range(n_col):
                far_part(t).start()

    parts[c] = jnp.sum(acc[...], axis=2)
    out_copies = []
    for t in range(1, n_col):
        out_copies.append(pltpu.make_async_remote_copy(
            src_ref=parts.at[c], dst_ref=parts.at[c],
            send_sem=part_send.at[t - 1], recv_sem=part_recv.at[t - 1],
            device_id={"col": other(c, t, n_col)}, device_id_type=MESH))
    for copy in out_copies:
        copy.start()
    for copy in sends:
        copy.wait_send()
    for t in range(reach):
        @pl.when((r - t >= 0) & (r < n_row - 1))
        def _():
            col_copy(r - t, 0, r).wait_send()
        @pl.when((r + t < n_row) & (r > 0))
        def _():
            col_copy(r + t, 1, r).wait_send()
    for copy in out_copies:
        copy.wait()
    planes[r] = jnp.sum(parts[0:n_col], axis=0)
    if moved:
        @pl.when(inner)
        def _():
            for t in range(n_col):
                far_part(t).wait_send()

        @pl.when(outer)
        def _():
            for t in range(n_col):
                far_part(t).wait_recv()
            planes[r] = planes[r] + jnp.sum(parts[n_col:2 * n_col], axis=0)
    plane_ref[...] = planes[r]
    plane_copies = []
    for t in range(1, n_row):
        plane_copies.append(pltpu.make_async_remote_copy(
            src_ref=planes.at[r], dst_ref=planes.at[r],
            send_sem=plane_send.at[t - 1], recv_sem=plane_recv.at[t - 1],
            device_id={"row": other(r, t, n_row)}, device_id_type=MESH))
    for copy in plane_copies:
        copy.start()
    for copy in plane_copies:
        copy.wait()
    total_ref[...] = jnp.full(total_ref.shape, jnp.sum(planes[...]), jnp.float32)


def on_device(n_row, n_col, tile_data, tile_cols):
    rows = tile_data.shape[0]
    slots = tile_data.shape[3]
    width = tile_data.shape[4]
    n_tiles = rows * slots
    tiles = tile_data.reshape(n_tiles, width, width)
    cols = jnp.pad(tile_cols.reshape(rows, slots), ((0, 0), (0, 128 - slots)), constant_values=-1)
    Y, X = plane_shape(n_col)
    n_far = max(n_col // n_row, 1)
    n_sends = 2 * (n_col + (X - 1) + (Y - 1)) + (X - 1) * (Y - 1) * 2 + (X - 1) + (Y - 1) + 8
    dma = pltpu.SemaphoreType.DMA
    plane, total = pl.pallas_call(
        functools.partial(kernel, n_row, n_col),
        out_shape=(jax.ShapeDtypeStruct((rows, width), jnp.float32),
                   jax.ShapeDtypeStruct((8, 128), jnp.float32)),
        in_specs=[pl.BlockSpec(memory_space=pl.ANY), pl.BlockSpec(memory_space=pl.ANY)],
        out_specs=(pl.BlockSpec(memory_space=pltpu.VMEM), pl.BlockSpec(memory_space=pltpu.VMEM)),
        scratch_shapes=[
            pltpu.VMEM((n_col * n_tiles + 1, width, width), jnp.bfloat16),
            pltpu.VMEM((n_row * n_tiles + 1, width, width), jnp.bfloat16),
            pltpu.VMEM((n_far * n_tiles + 1, width, width), jnp.bfloat16),
            pltpu.VMEM((n_col, rows, 128), jnp.int32),
            pltpu.VMEM((n_row, rows, 128), jnp.int32),
            pltpu.VMEM((n_far, rows, 128), jnp.int32),
            pltpu.SMEM((n_col, rows, 128), jnp.int32),
            pltpu.SMEM((n_row, rows, 128), jnp.int32),
            pltpu.SMEM((n_far, rows, 128), jnp.int32),
            pltpu.VMEM((rows, width, width), jnp.float32),
            pltpu.VMEM((rows, width, width), jnp.float32),
            pltpu.VMEM((2 * n_col, rows, width), jnp.float32),
            pltpu.VMEM((n_row, rows, width), jnp.float32),
            dma((6,)), dma((3,)),
            dma((n_sends,)), dma((n_col, 2)),
            dma((n_row, 2)), dma((n_row,)),
            dma((n_col + n_row - 2,)), dma((n_col + n_row - 2,)),
            dma((n_col - 1,)), dma((n_col - 1,)),
            dma((max(n_row - 1, 1),)), dma((max(n_row - 1, 1),)),
            dma((n_far, 2, X + Y)), dma((n_far, 2)),
            dma((n_far, n_col - 1)), dma((n_far,)),
            dma((n_col,)), dma((n_col,)),
        ],
        compiler_params=pltpu.CompilerParams(collective_id=0, has_side_effects=True),
    )(tiles, cols)
    share = width // n_col
    start = lax.axis_index("col") * share
    shares = lax.dynamic_slice_in_dim(plane, start, share, 1).reshape(rows, 1, share)
    vertices = rows * n_row * width
    return shares * vertex_scale, total[0, 0] * (total_scale / vertices)


def solution(mesh):
    return jax.shard_map(
        functools.partial(on_device, mesh.shape["row"], mesh.shape["col"]),
        mesh=mesh,
        in_specs=(P(None, "row", "col", None, None, None), P(None, "row", "col", None)),
        out_specs=(P(None, "row", "col"), P()),
        check_vma=False,
    )
```

```python
import functools
import math

import jax
import jax.numpy as jnp
from jax import lax
from jax.experimental import pallas as pl
from jax.experimental.pallas import tpu as pltpu
from jax.sharding import PartitionSpec as P

MESH = pl.DeviceIdType.MESH
vertex_scale = 2.0 ** (-14)
total_scale = 2.0 ** (-12)


def plane_shape(n_col):
    chips = n_col // 2
    side = math.isqrt(chips)
    return (side, side) if side * side == chips else (1, chips)


def kernel(n_row, n_col, tiles, cols_ref, share_ref, total_ref,
           row_buf, col_buf, far_buf, row_idx, col_idx, far_idx, row_smem, col_smem, far_smem,
           acc, far_acc, parts, sums,
           load_sem, smem_sem, row_send, row_recv, col_send, col_recv,
           idx_send, idx_recv, part_send, part_recv, sum_send, sum_recv,
           far_send, far_recv, fidx_send, fidx_recv, fpart_send, fpart_recv):
    r = lax.axis_index("row")
    c = lax.axis_index("col")
    n_tiles = tiles.shape[0]
    half = n_tiles // 2
    rows = acc.shape[0]
    slots = n_tiles // rows
    width = tiles.shape[1]
    zero = n_col * n_tiles
    moved = n_row >= 4 and n_col % n_row == 0
    reach = n_row - 2 if moved else n_row - 1
    n_far = max(n_col // n_row, 1)
    far_zero = n_far * n_tiles
    low = r < n_row // 2
    inner = (r == 1) | (r == n_row - 2)
    outer = (r == 0) | (r == n_row - 1)
    far_left = jnp.where(low, 0, n_row - 1)
    far_middle = n_row - 1 - far_left
    neighbour = jnp.where(low, 1 - r, 2 * n_row - 3 - r)
    Y, X = plane_shape(n_col)
    u = c % 2
    x = (c // 2) % X
    y = c // (2 * X)

    def col_of(yy, xx, uu):
        return (yy * X + xx) * 2 + uu

    def row_block(cc, h):
        return row_buf.at[pl.ds(cc * n_tiles + h * half, half)]

    def col_block(rr):
        return col_buf.at[pl.ds(rr * n_tiles, n_tiles)]

    load_row = pltpu.make_async_copy(tiles, row_buf.at[pl.ds(c * n_tiles, n_tiles)], load_sem.at[0])
    load_row.start()
    load_col = pltpu.make_async_copy(tiles, col_block(r), load_sem.at[1])
    load_col.start()
    load_ri = pltpu.make_async_copy(cols_ref, row_idx.at[c], load_sem.at[2])
    load_ri.start()
    load_ci = pltpu.make_async_copy(cols_ref, col_idx.at[r], load_sem.at[3])
    load_ci.start()

    barrier = pltpu.get_barrier_semaphore()
    for t in range(1, n_col):
        pl.semaphore_signal(barrier, inc=1, device_id={"col": lax.rem(c + t, n_col)}, device_id_type=MESH)
    for t in range(1, n_row):
        pl.semaphore_signal(barrier, inc=1, device_id={"row": lax.rem(r + t, n_row)}, device_id_type=MESH)
    row_buf[zero] = jnp.zeros(row_buf.shape[1:], row_buf.dtype)
    far_buf[far_zero] = jnp.zeros(far_buf.shape[1:], far_buf.dtype)
    col_buf[n_row * n_tiles] = jnp.zeros(col_buf.shape[1:], col_buf.dtype)
    acc[...] = jnp.zeros_like(acc)
    far_acc[...] = jnp.zeros_like(far_acc)
    load_row.wait()
    load_col.wait()
    pl.semaphore_wait(barrier, n_col + n_row - 2)

    sends = []

    def send_row(cc, h, dest):
        copy = pltpu.make_async_remote_copy(
            src_ref=row_block(cc, h), dst_ref=row_block(cc, h),
            send_sem=row_send.at[len(sends)], recv_sem=row_recv.at[cc, h],
            device_id={"col": dest}, device_id_type=MESH)
        copy.start()
        sends.append(copy)

    def got_row(cc, h):
        pltpu.make_async_remote_copy(
            src_ref=row_block(cc, h), dst_ref=row_block(cc, h),
            send_sem=row_send.at[0], recv_sem=row_recv.at[cc, h],
            device_id={"col": lax.rem(c + 1, n_col)}, device_id_type=MESH).wait_recv()

    def col_copy(rr, way, dest):
        return pltpu.make_async_remote_copy(
            src_ref=col_block(rr), dst_ref=col_block(rr),
            send_sem=col_send.at[rr, way], recv_sem=col_recv.at[rr],
            device_id={"row": dest}, device_id_type=MESH)

    def other(value, t, n):
        return lax.rem(value + t, n)

    def pass_on(t):
        up, down = r - t, r + t
        if t > 0:
            @pl.when(up >= 0)
            def _():
                col_copy(up, 0, r).wait_recv()
        if t < reach:
            @pl.when((up >= 0) & (r < n_row - 1))
            def _():
                col_copy(up, 0, r + 1).start()
        if t > 0:
            @pl.when(down < n_row)
            def _():
                col_copy(down, 1, r).wait_recv()
        if t < reach:
            @pl.when((down < n_row) & (r > 0))
            def _():
                col_copy(down, 1, r - 1).start()

    pass_on(0)
    xs = [col_of(y, other(x, t, X), u) for t in range(1, X)]
    ys = [col_of(other(y, t, Y), x, u) for t in range(1, Y)]
    for dest in xs:
        send_row(c, 0, dest)
    for dest in ys:
        send_row(c, 1, dest)
    load_ri.wait()
    load_ci.wait()
    idx_copies = []
    for t in range(1, n_col):
        idx_copies.append(pltpu.make_async_remote_copy(
            src_ref=row_idx.at[c], dst_ref=row_idx.at[c],
            send_sem=idx_send.at[t - 1], recv_sem=idx_recv.at[t - 1],
            device_id={"col": other(c, t, n_col)}, device_id_type=MESH))
    for t in range(1, n_row):
        idx_copies.append(pltpu.make_async_remote_copy(
            src_ref=col_idx.at[r], dst_ref=col_idx.at[r],
            send_sem=idx_send.at[n_col - 2 + t], recv_sem=idx_recv.at[n_col - 2 + t],
            device_id={"row": other(r, t, n_row)}, device_id_type=MESH))
    for copy in idx_copies:
        copy.start()
    for dest in ys:
        send_row(c, 0, dest)
    for dest in xs:
        send_row(c, 1, dest)
    for h in range(2):
        send_row(c, h, c + 1 - 2 * u)
    for t in range(1, max(X, Y)):
        if t < X:
            cc = col_of(y, other(x, t, X), u)
            got_row(cc, 0)
            for dest in ys:
                send_row(cc, 0, dest)
        if t < Y:
            cc = col_of(other(y, t, Y), x, u)
            got_row(cc, 1)
            for dest in xs:
                send_row(cc, 1, dest)
    for t in range(1, X):
        send_row(col_of(y, other(x, t, X), u), 0, c + 1 - 2 * u)
    for t in range(1, Y):
        send_row(col_of(other(y, t, Y), x, u), 1, c + 1 - 2 * u)
    if n_row > 1:
        pass_on(1)

    ways = X + Y

    def far_block(e, h):
        return far_buf.at[pl.ds(e * n_tiles + h * half, half)]

    def far_copy(e, h, way, dest, source=None):
        return pltpu.make_async_remote_copy(
            src_ref=far_block(e, h) if source is None else source, dst_ref=far_block(e, h),
            send_sem=far_send.at[e, h, way], recv_sem=far_recv.at[e, h],
            device_id={"col": dest}, device_id_type=MESH)

    def far_index(e, t):
        return pltpu.make_async_remote_copy(
            src_ref=far_idx.at[e], dst_ref=far_idx.at[e],
            send_sem=fidx_send.at[e, t - 1], recv_sem=fidx_recv.at[e],
            device_id={"col": other(c, t, n_col)}, device_id_type=MESH)

    def far_tiles(e):
        return pltpu.make_async_copy(
            col_buf.at[pl.ds(far_left * n_tiles, n_tiles)],
            far_buf.at[pl.ds(e * n_tiles, n_tiles)], load_sem.at[4])

    def far_place(e):
        cc = e * n_row + far_middle
        return cc, (cc % 2) == u, ((cc // 2) % X) == x, (cc // (2 * X)) == y

    partner = c + 1 - 2 * u
    to_x = [(t, dest) for t, dest in enumerate(xs, 1)]
    to_y = [(X - 1 + t, dest) for t, dest in enumerate(ys, 1)]

    def far_source():
        for e in range(n_far):
            cc, same_u, same_x, same_y = far_place(e)

            @pl.when(inner & (cc == c))
            def _():
                source = col_buf.at[pl.ds(far_left * n_tiles, half)]
                source2 = col_buf.at[pl.ds(far_left * n_tiles + half, half)]
                for way, dest in to_x:
                    far_copy(e, 0, way, dest, source).start()
                for way, dest in to_y:
                    far_copy(e, 1, way, dest, source2).start()
                for way, dest in to_y:
                    far_copy(e, 0, way, dest, source).start()
                for way, dest in to_x:
                    far_copy(e, 1, way, dest, source2).start()
                far_copy(e, 0, 0, partner, source).start()
                far_copy(e, 1, 0, partner, source2).start()
                far_tiles(e).start()
                index = pltpu.make_async_copy(col_idx.at[far_left], far_idx.at[e], load_sem.at[5])
                index.start()
                index.wait()
                for t in range(1, n_col):
                    far_index(e, t).start()

    def far_relay(first):
        for e in range(n_far):
            cc, same_u, same_x, same_y = far_place(e)
            here = inner & same_u & (cc != c)

            @pl.when(here & same_y)
            def _():
                h = 0 if first else 1
                far_copy(e, h, 0, partner).wait_recv()
                if first:
                    for way, dest in to_y:
                        far_copy(e, 0, way, dest).start()
                far_copy(e, h, 0, partner).start()

            @pl.when(here & same_x)
            def _():
                h = 1 if first else 0
                far_copy(e, h, 0, partner).wait_recv()
                if first:
                    for way, dest in to_x:
                        far_copy(e, 1, way, dest).start()
                far_copy(e, h, 0, partner).start()

            if not first:
                @pl.when(here & jnp.logical_not(same_x | same_y))
                def _():
                    for h in range(2):
                        far_copy(e, h, 0, partner).wait_recv()
                        far_copy(e, h, 0, partner).start()

    def far_end():
        for e in range(n_far):
            cc, same_u, same_x, same_y = far_place(e)

            @pl.when(inner & jnp.logical_not(same_u))
            def _():
                for h in range(2):
                    far_copy(e, h, 0, partner).wait_recv()

            @pl.when(inner & (cc != c))
            def _():
                far_index(e, 1).wait_recv()

            @pl.when(inner & (cc == c))
            def _():
                far_tiles(e).wait()
                for t in range(1, n_col):
                    far_index(e, t).wait_send()
                for h in range(2):
                    for way in range(ways - 1):
                        far_copy(e, h, way, partner).wait_send()

            @pl.when(inner & same_u & (cc != c))
            def _():
                for h in range(2):
                    far_copy(e, h, 0, partner).wait_send()

            @pl.when(inner & same_u & (cc != c) & same_y)
            def _():
                for way, dest in to_y:
                    far_copy(e, 0, way, dest).wait_send()

            @pl.when(inner & same_u & (cc != c) & same_x)
            def _():
                for way, dest in to_x:
                    far_copy(e, 1, way, dest).wait_send()

    for copy in idx_copies:
        copy.wait()
    if moved:
        far_source()
    for t in range(1, X):
        cc = col_of(y, other(x, t, X), u)
        got_row(cc, 1)
        send_row(cc, 1, c + 1 - 2 * u)
    for t in range(1, Y):
        cc = col_of(other(y, t, Y), x, u)
        got_row(cc, 0)
        send_row(cc, 0, c + 1 - 2 * u)
    for tx in range(1, X):
        for ty in range(1, Y):
            cc = col_of(other(y, ty, Y), other(x, tx, X), u)
            for h in range(2):
                got_row(cc, h)
                send_row(cc, h, c + 1 - 2 * u)
    for m in range(n_col // 2):
        for h in range(2):
            got_row(2 * m + 1 - u, h)
    to_smem = [pltpu.make_async_copy(row_idx, row_smem, smem_sem.at[0]),
               pltpu.make_async_copy(col_idx, col_smem, smem_sem.at[1])]
    for copy in to_smem:
        copy.start()
    for copy in to_smem:
        copy.wait()

    def unit(rr, left_slot, left_buf, left_zero, own_slot, own_buf, own_zero, own_base, total):
        def step(b, carry):
            middle = b * n_row + rr
            block = lax.rem(middle, n_col)
            left = []
            for a in range(rows):
                index = jnp.int32(left_zero)
                for s in range(slots):
                    held, base = left_slot(block, a, s)
                    index = jnp.where(held == middle, base + a * slots + s, index)
                left.append(left_buf[index])
            left = jnp.concatenate(left, axis=0)
            right = jnp.concatenate(
                [col_buf[rr * n_tiles + b * slots + s] for s in range(slots)], axis=1)
            paths = jnp.dot(left, right, preferred_element_type=jnp.float32)
            for a in range(rows):
                value = total[a]
                for s in range(slots):
                    target = col_smem[rr, s, b]
                    index = jnp.int32(own_zero)
                    for q in range(slots):
                        own = own_slot(a, q)
                        index = jnp.where((own == target) & (target >= 0), own_base + a * slots + q, index)
                    value = value + paths[a * width:(a + 1) * width, s * width:(s + 1) * width] * (
                        own_buf[index].astype(jnp.float32))
                total[a] = value
            return carry
        lax.fori_loop(0, rows, step, 0)

    def near_unit(rr):
        unit(rr, lambda block, a, s: (row_smem[block, s, a], block * n_tiles), row_buf, zero,
             lambda a, q: row_smem[c, q, a], row_buf, zero, c * n_tiles, acc)

    def far_unit():
        unit(far_middle,
             lambda block, a, s: (far_smem[block // n_row, s, a], (block // n_row) * n_tiles),
             far_buf, far_zero,
             lambda a, q: col_smem[far_left, q, a], col_buf, n_row * n_tiles,
             far_left * n_tiles, far_acc)

    def units(t):
        @pl.when(r - t >= 0)
        def _():
            near_unit(r - t)
        @pl.when(r + t < n_row)
        def _():
            near_unit(r + t)

    for t in range(2, reach):
        pass_on(t)
    if moved:
        far_relay(True)
    near_unit(r)
    for t in range(1, reach):
        units(t)
    if moved:
        far_relay(False)
    if reach > 1:
        pass_on(reach)
    if reach > 0:
        units(reach)
    if moved:
        far_end()

        @pl.when(inner)
        def _():
            copy = pltpu.make_async_copy(far_idx, far_smem, smem_sem.at[2])
            copy.start()
            copy.wait()
            far_unit()

    def far_part(t):
        return pltpu.make_async_remote_copy(
            src_ref=parts.at[n_col + c], dst_ref=parts.at[n_col + c],
            send_sem=fpart_send.at[t], recv_sem=fpart_recv.at[t],
            device_id={"row": neighbour, "col": other(c, t, n_col)}, device_id_type=MESH)

    n_all = n_row * n_col
    me = r * n_col + c
    counts = jnp.sum(acc[...], axis=2)
    parts[c] = counts
    if moved:
        far_counts = jnp.sum(far_acc[...], axis=2)

        @pl.when(inner)
        def _():
            parts[n_col + c] = far_counts

        counts = counts + far_counts
    sums[me] = jnp.sum(counts, axis=0, keepdims=True)

    def send_sum(t, carry):
        dest = lax.rem(me + t, n_all)
        pltpu.make_async_remote_copy(
            src_ref=sums.at[me], dst_ref=sums.at[me],
            send_sem=sum_send.at[0], recv_sem=sum_recv.at[0],
            device_id={"row": dest // n_col, "col": lax.rem(dest, n_col)}, device_id_type=MESH).start()
        return carry

    lax.fori_loop(1, n_all, send_sum, 0)
    out_copies = []
    for t in range(1, n_col):
        out_copies.append(pltpu.make_async_remote_copy(
            src_ref=parts.at[c], dst_ref=parts.at[c],
            send_sem=part_send.at[t - 1], recv_sem=part_recv.at[t - 1],
            device_id={"col": other(c, t, n_col)}, device_id_type=MESH))
    for copy in out_copies:
        copy.start()
    if moved:
        @pl.when(inner)
        def _():
            for t in range(n_col):
                far_part(t).start()
    for copy in sends:
        copy.wait_send()
    for t in range(reach):
        @pl.when((r - t >= 0) & (r < n_row - 1))
        def _():
            col_copy(r - t, 0, r).wait_send()
        @pl.when((r + t < n_row) & (r > 0))
        def _():
            col_copy(r + t, 1, r).wait_send()
    for copy in out_copies:
        copy.wait()
    if moved:
        @pl.when(inner)
        def _():
            for t in range(n_col):
                far_part(t).wait_send()
            parts[n_col] = jnp.zeros(parts.shape[1:], parts.dtype)

        @pl.when(outer)
        def _():
            for t in range(n_col):
                far_part(t).wait_recv()
            parts[n_col] = jnp.sum(parts[n_col:2 * n_col], axis=0)
    plane = jnp.sum(parts[0:n_col], axis=0)
    if moved:
        @pl.when(jnp.logical_not(inner | outer))
        def _():
            parts[n_col] = jnp.zeros(parts.shape[1:], parts.dtype)
        plane = plane + parts[n_col]
    share = width // n_col
    mine = pltpu.roll(plane, lax.rem(width - c * share, width), 1)
    for a in range(rows):
        share_ref[a] = mine[a:a + 1, 0:share] * vertex_scale
    everyone = pltpu.make_async_remote_copy(
        src_ref=sums.at[pl.ds(0, n_all - 1)], dst_ref=sums.at[pl.ds(0, n_all - 1)],
        send_sem=sum_send.at[0], recv_sem=sum_recv.at[0],
        device_id={"col": lax.rem(c + 1, n_col)}, device_id_type=MESH)
    everyone.wait_send()
    everyone.wait_recv()
    total_ref[0, 0] = jnp.sum(sums[...]) * (total_scale / (rows * n_row * width))


def on_device(n_row, n_col, tile_data, tile_cols):
    rows = tile_data.shape[0]
    slots = tile_data.shape[3]
    width = tile_data.shape[4]
    n_tiles = rows * slots
    tiles = tile_data.reshape(n_tiles, width, width)
    cols = jnp.transpose(tile_cols.reshape(rows, slots))
    Y, X = plane_shape(n_col)
    n_far = max(n_col // n_row, 1)
    n_sends = 2 * (n_col + (X - 1) + (Y - 1)) + (X - 1) * (Y - 1) * 2 + (X - 1) + (Y - 1) + 8
    dma = pltpu.SemaphoreType.DMA
    share = width // n_col
    shares, total = pl.pallas_call(
        functools.partial(kernel, n_row, n_col),
        out_shape=(jax.ShapeDtypeStruct((rows, 1, share), jnp.float32),
                   jax.ShapeDtypeStruct((1, 1), jnp.float32)),
        in_specs=[pl.BlockSpec(memory_space=pl.ANY), pl.BlockSpec(memory_space=pl.ANY)],
        out_specs=(pl.BlockSpec(memory_space=pltpu.VMEM), pl.BlockSpec(memory_space=pltpu.SMEM)),
        scratch_shapes=[
            pltpu.VMEM((n_col * n_tiles + 1, width, width), jnp.bfloat16),
            pltpu.VMEM((n_row * n_tiles + 1, width, width), jnp.bfloat16),
            pltpu.VMEM((n_far * n_tiles + 1, width, width), jnp.bfloat16),
            pltpu.VMEM((n_col, slots, rows), jnp.int32),
            pltpu.VMEM((n_row, slots, rows), jnp.int32),
            pltpu.VMEM((n_far, slots, rows), jnp.int32),
            pltpu.SMEM((n_col, slots, rows), jnp.int32),
            pltpu.SMEM((n_row, slots, rows), jnp.int32),
            pltpu.SMEM((n_far, slots, rows), jnp.int32),
            pltpu.VMEM((rows, width, width), jnp.float32),
            pltpu.VMEM((rows, width, width), jnp.float32),
            pltpu.VMEM((2 * n_col, rows, width), jnp.float32),
            pltpu.VMEM((n_row * n_col, 1, width), jnp.float32),
            dma((6,)), dma((3,)),
            dma((n_sends,)), dma((n_col, 2)),
            dma((n_row, 2)), dma((n_row,)),
            dma((n_col + n_row - 2,)), dma((n_col + n_row - 2,)),
            dma((n_col - 1,)), dma((n_col - 1,)),
            dma((1,)), dma((1,)),
            dma((n_far, 2, X + Y)), dma((n_far, 2)),
            dma((n_far, n_col - 1)), dma((n_far,)),
            dma((n_col,)), dma((n_col,)),
        ],
        compiler_params=pltpu.CompilerParams(collective_id=0, has_side_effects=True),
    )(tiles, cols)
    return shares, total[0, 0]


def solution(mesh):
    return jax.shard_map(
        functools.partial(on_device, mesh.shape["row"], mesh.shape["col"]),
        mesh=mesh,
        in_specs=(P(None, "row", "col", None, None, None), P(None, "row", "col", None)),
        out_specs=(P(None, "row", "col"), P()),
        check_vma=False,
    )
```

```python
import functools
import math

import jax
import jax.numpy as jnp
from jax import lax
from jax.experimental import pallas as pl
from jax.experimental.pallas import tpu as pltpu
from jax.sharding import PartitionSpec as P

MESH = pl.DeviceIdType.MESH
vertex_scale = 2.0 ** (-14)
total_scale = 2.0 ** (-12)


def plane_shape(n_col):
    chips = n_col // 2
    side = math.isqrt(chips)
    return (side, side) if side * side == chips else (1, chips)


def kernel(n_row, n_col, tiles, cols_ref, share_ref, total_ref,
           row_buf, col_buf, far_buf, row_idx, col_idx, far_idx, row_smem, col_smem, far_smem,
           acc, far_acc, parts, sums,
           load_sem, smem_sem, row_send, row_recv, col_send, col_recv,
           idx_send, idx_recv, part_send, part_recv, sum_send, sum_recv,
           far_send, far_recv, fidx_send, fidx_recv, fpart_send, fpart_recv):
    r = lax.axis_index("row")
    c = lax.axis_index("col")
    n_tiles = tiles.shape[0]
    half = n_tiles // 2
    rows = acc.shape[0]
    slots = n_tiles // rows
    width = tiles.shape[1]
    zero = n_col * n_tiles
    moved = n_row >= 4 and n_col % n_row == 0
    reach = n_row - 2 if moved else n_row - 1
    n_far = max(n_col // n_row, 1)
    far_zero = n_far * n_tiles
    low = r < n_row // 2
    inner = (r == 1) | (r == n_row - 2)
    outer = (r == 0) | (r == n_row - 1)
    far_left = jnp.where(low, 0, n_row - 1)
    far_middle = n_row - 1 - far_left
    neighbour = jnp.where(low, 1 - r, 2 * n_row - 3 - r)
    Y, X = plane_shape(n_col)
    u = c % 2
    x = (c // 2) % X
    y = c // (2 * X)

    def col_of(yy, xx, uu):
        return (yy * X + xx) * 2 + uu

    def row_block(cc, h):
        return row_buf.at[pl.ds(cc * n_tiles + h * half, half)]

    def col_block(rr):
        return col_buf.at[pl.ds(rr * n_tiles, n_tiles)]

    load_row = pltpu.make_async_copy(tiles, row_buf.at[pl.ds(c * n_tiles, n_tiles)], load_sem.at[0])
    load_row.start()
    load_col = pltpu.make_async_copy(tiles, col_block(r), load_sem.at[1])
    load_col.start()
    load_ri = pltpu.make_async_copy(cols_ref, row_idx.at[c], load_sem.at[2])
    load_ri.start()
    load_ci = pltpu.make_async_copy(cols_ref, col_idx.at[r], load_sem.at[3])
    load_ci.start()

    barrier = pltpu.get_barrier_semaphore()
    for t in range(1, n_col):
        pl.semaphore_signal(barrier, inc=1, device_id={"col": lax.rem(c + t, n_col)}, device_id_type=MESH)
    for t in range(1, n_row):
        pl.semaphore_signal(barrier, inc=1, device_id={"row": lax.rem(r + t, n_row)}, device_id_type=MESH)
    row_buf[zero] = jnp.zeros(row_buf.shape[1:], row_buf.dtype)
    far_buf[far_zero] = jnp.zeros(far_buf.shape[1:], far_buf.dtype)
    col_buf[n_row * n_tiles] = jnp.zeros(col_buf.shape[1:], col_buf.dtype)
    acc[...] = jnp.zeros_like(acc)
    far_acc[...] = jnp.zeros_like(far_acc)
    load_row.wait()
    load_col.wait()
    pl.semaphore_wait(barrier, n_col + n_row - 2)

    sends = []

    def send_row(cc, h, dest):
        copy = pltpu.make_async_remote_copy(
            src_ref=row_block(cc, h), dst_ref=row_block(cc, h),
            send_sem=row_send.at[len(sends)], recv_sem=row_recv.at[cc, h],
            device_id={"col": dest}, device_id_type=MESH)
        copy.start()
        sends.append(copy)

    def got_row(cc, h):
        pltpu.make_async_remote_copy(
            src_ref=row_block(cc, h), dst_ref=row_block(cc, h),
            send_sem=row_send.at[0], recv_sem=row_recv.at[cc, h],
            device_id={"col": lax.rem(c + 1, n_col)}, device_id_type=MESH).wait_recv()

    def col_copy(rr, way, dest):
        return pltpu.make_async_remote_copy(
            src_ref=col_block(rr), dst_ref=col_block(rr),
            send_sem=col_send.at[rr, way], recv_sem=col_recv.at[rr],
            device_id={"row": dest}, device_id_type=MESH)

    def other(value, t, n):
        return lax.rem(value + t, n)

    def pass_on(t):
        up, down = r - t, r + t
        if t > 0:
            @pl.when(up >= 0)
            def _():
                col_copy(up, 0, r).wait_recv()
        if t < reach:
            @pl.when((up >= 0) & (r < n_row - 1))
            def _():
                col_copy(up, 0, r + 1).start()
        if t > 0:
            @pl.when(down < n_row)
            def _():
                col_copy(down, 1, r).wait_recv()
        if t < reach:
            @pl.when((down < n_row) & (r > 0))
            def _():
                col_copy(down, 1, r - 1).start()

    pass_on(0)
    xs = [col_of(y, other(x, t, X), u) for t in range(1, X)]
    ys = [col_of(other(y, t, Y), x, u) for t in range(1, Y)]
    for dest in xs:
        send_row(c, 0, dest)
    for dest in ys:
        send_row(c, 1, dest)
    load_ri.wait()
    load_ci.wait()
    idx_copies = []
    for t in range(1, n_col):
        idx_copies.append(pltpu.make_async_remote_copy(
            src_ref=row_idx.at[c], dst_ref=row_idx.at[c],
            send_sem=idx_send.at[t - 1], recv_sem=idx_recv.at[t - 1],
            device_id={"col": other(c, t, n_col)}, device_id_type=MESH))
    for t in range(1, n_row):
        idx_copies.append(pltpu.make_async_remote_copy(
            src_ref=col_idx.at[r], dst_ref=col_idx.at[r],
            send_sem=idx_send.at[n_col - 2 + t], recv_sem=idx_recv.at[n_col - 2 + t],
            device_id={"row": other(r, t, n_row)}, device_id_type=MESH))
    for copy in idx_copies:
        copy.start()
    for dest in ys:
        send_row(c, 0, dest)
    for dest in xs:
        send_row(c, 1, dest)
    for h in range(2):
        send_row(c, h, c + 1 - 2 * u)
    for t in range(1, max(X, Y)):
        if t < X:
            cc = col_of(y, other(x, t, X), u)
            got_row(cc, 0)
            for dest in ys:
                send_row(cc, 0, dest)
        if t < Y:
            cc = col_of(other(y, t, Y), x, u)
            got_row(cc, 1)
            for dest in xs:
                send_row(cc, 1, dest)
    for t in range(1, X):
        send_row(col_of(y, other(x, t, X), u), 0, c + 1 - 2 * u)
    for t in range(1, Y):
        send_row(col_of(other(y, t, Y), x, u), 1, c + 1 - 2 * u)
    if n_row > 1:
        pass_on(1)

    ways = X + Y

    def far_block(e, h):
        return far_buf.at[pl.ds(e * n_tiles + h * half, half)]

    def far_copy(e, h, way, dest, source=None):
        return pltpu.make_async_remote_copy(
            src_ref=far_block(e, h) if source is None else source, dst_ref=far_block(e, h),
            send_sem=far_send.at[e, h, way], recv_sem=far_recv.at[e, h],
            device_id={"col": dest}, device_id_type=MESH)

    def far_index(e, t):
        return pltpu.make_async_remote_copy(
            src_ref=far_idx.at[e], dst_ref=far_idx.at[e],
            send_sem=fidx_send.at[e, t - 1], recv_sem=fidx_recv.at[e],
            device_id={"col": other(c, t, n_col)}, device_id_type=MESH)

    def far_tiles(e):
        return pltpu.make_async_copy(
            col_buf.at[pl.ds(far_left * n_tiles, n_tiles)],
            far_buf.at[pl.ds(e * n_tiles, n_tiles)], load_sem.at[4])

    def far_place(e):
        cc = e * n_row + far_middle
        return cc, (cc % 2) == u, ((cc // 2) % X) == x, (cc // (2 * X)) == y

    partner = c + 1 - 2 * u
    to_x = [(t, dest) for t, dest in enumerate(xs, 1)]
    to_y = [(X - 1 + t, dest) for t, dest in enumerate(ys, 1)]

    def far_source():
        for e in range(n_far):
            cc, same_u, same_x, same_y = far_place(e)

            @pl.when(inner & (cc == c))
            def _():
                source = col_buf.at[pl.ds(far_left * n_tiles, half)]
                source2 = col_buf.at[pl.ds(far_left * n_tiles + half, half)]
                for way, dest in to_x:
                    far_copy(e, 0, way, dest, source).start()
                for way, dest in to_y:
                    far_copy(e, 1, way, dest, source2).start()
                for way, dest in to_y:
                    far_copy(e, 0, way, dest, source).start()
                for way, dest in to_x:
                    far_copy(e, 1, way, dest, source2).start()
                far_copy(e, 0, 0, partner, source).start()
                far_copy(e, 1, 0, partner, source2).start()
                far_tiles(e).start()
                index = pltpu.make_async_copy(col_idx.at[far_left], far_idx.at[e], load_sem.at[5])
                index.start()
                index.wait()
                for t in range(1, n_col):
                    far_index(e, t).start()

    def far_relay(first):
        for e in range(n_far):
            cc, same_u, same_x, same_y = far_place(e)
            here = inner & same_u & (cc != c)

            @pl.when(here & same_y)
            def _():
                h = 0 if first else 1
                far_copy(e, h, 0, partner).wait_recv()
                if first:
                    for way, dest in to_y:
                        far_copy(e, 0, way, dest).start()
                far_copy(e, h, 0, partner).start()

            @pl.when(here & same_x)
            def _():
                h = 1 if first else 0
                far_copy(e, h, 0, partner).wait_recv()
                if first:
                    for way, dest in to_x:
                        far_copy(e, 1, way, dest).start()
                far_copy(e, h, 0, partner).start()

            if not first:
                @pl.when(here & jnp.logical_not(same_x | same_y))
                def _():
                    for h in range(2):
                        far_copy(e, h, 0, partner).wait_recv()
                        far_copy(e, h, 0, partner).start()

    def far_end():
        for e in range(n_far):
            cc, same_u, same_x, same_y = far_place(e)

            @pl.when(inner & jnp.logical_not(same_u))
            def _():
                for h in range(2):
                    far_copy(e, h, 0, partner).wait_recv()

            @pl.when(inner & (cc == c))
            def _():
                far_tiles(e).wait()
                for t in range(1, n_col):
                    far_index(e, t).wait_send()
                for h in range(2):
                    for way in range(ways - 1):
                        far_copy(e, h, way, partner).wait_send()

            @pl.when(inner & same_u & (cc != c))
            def _():
                for h in range(2):
                    far_copy(e, h, 0, partner).wait_send()

            @pl.when(inner & same_u & (cc != c) & same_y)
            def _():
                for way, dest in to_y:
                    far_copy(e, 0, way, dest).wait_send()

            @pl.when(inner & same_u & (cc != c) & same_x)
            def _():
                for way, dest in to_x:
                    far_copy(e, 1, way, dest).wait_send()

    for copy in idx_copies:
        copy.wait()
    to_smem = [pltpu.make_async_copy(row_idx, row_smem, smem_sem.at[0]),
               pltpu.make_async_copy(col_idx, col_smem, smem_sem.at[1])]
    for copy in to_smem:
        copy.start()
    if moved:
        far_source()
    for t in range(1, X):
        cc = col_of(y, other(x, t, X), u)
        got_row(cc, 1)
        send_row(cc, 1, c + 1 - 2 * u)
    for t in range(1, Y):
        cc = col_of(other(y, t, Y), x, u)
        got_row(cc, 0)
        send_row(cc, 0, c + 1 - 2 * u)
    for tx in range(1, X):
        for ty in range(1, Y):
            cc = col_of(other(y, ty, Y), other(x, tx, X), u)
            for h in range(2):
                got_row(cc, h)
                send_row(cc, h, c + 1 - 2 * u)
    for m in range(n_col // 2):
        for h in range(2):
            got_row(2 * m + 1 - u, h)
    for copy in to_smem:
        copy.wait()

    def unit(rr, left_slot, left_buf, left_zero, own_slot, own_buf, own_zero, own_base, total):
        def step(b, carry):
            middle = b * n_row + rr
            block = lax.rem(middle, n_col)
            left = []
            for a in range(rows):
                index = jnp.int32(left_zero)
                for s in range(slots):
                    held, base = left_slot(block, a, s)
                    index = jnp.where(held == middle, base + a * slots + s, index)
                left.append(left_buf[index])
            right = jnp.concatenate(
                [col_buf[rr * n_tiles + b * slots + s] for s in range(slots)], axis=1)
            own_rows = []
            for a in range(rows):
                pair = []
                for s in range(slots):
                    target = col_smem[rr, s, b]
                    index = jnp.int32(own_zero)
                    for q in range(slots):
                        own = own_slot(a, q)
                        index = jnp.where((own == target) & (target >= 0), own_base + a * slots + q, index)
                    pair.append(own_buf[index])
                own_rows.append(jnp.concatenate(pair, axis=1))
            common = lax.dot_general(
                jnp.concatenate(own_rows, axis=0), right, (((1,), (1,)), ((), ())),
                preferred_element_type=jnp.float32)
            for a in range(rows):
                total[a] += common[a * width:(a + 1) * width] * left[a].astype(jnp.float32)
            return carry
        lax.fori_loop(0, rows, step, 0)

    def near_unit(rr):
        unit(rr, lambda block, a, s: (row_smem[block, s, a], block * n_tiles), row_buf, zero,
             lambda a, q: row_smem[c, q, a], row_buf, zero, c * n_tiles, acc)

    def far_unit():
        unit(far_middle,
             lambda block, a, s: (far_smem[block // n_row, s, a], (block // n_row) * n_tiles),
             far_buf, far_zero,
             lambda a, q: col_smem[far_left, q, a], col_buf, n_row * n_tiles,
             far_left * n_tiles, far_acc)

    def units(t):
        @pl.when(r - t >= 0)
        def _():
            near_unit(r - t)
        @pl.when(r + t < n_row)
        def _():
            near_unit(r + t)

    for t in range(2, reach):
        pass_on(t)
    if moved:
        far_relay(True)
    near_unit(r)
    for t in range(1, reach):
        units(t)
    far_to_smem = pltpu.make_async_copy(far_idx, far_smem, smem_sem.at[2])
    if moved:
        far_relay(False)
        for e in range(n_far):
            @pl.when(inner & (far_place(e)[0] != c))
            def _():
                far_index(e, 1).wait_recv()

        @pl.when(inner)
        def _():
            far_to_smem.start()
    if reach > 1:
        pass_on(reach)
    if reach > 0:
        units(reach)
    if moved:
        far_end()

        @pl.when(inner)
        def _():
            far_to_smem.wait()
            far_unit()

    def far_part(t):
        return pltpu.make_async_remote_copy(
            src_ref=parts.at[n_col + c], dst_ref=parts.at[n_col + c],
            send_sem=fpart_send.at[t], recv_sem=fpart_recv.at[t],
            device_id={"row": neighbour, "col": other(c, t, n_col)}, device_id_type=MESH)

    n_all = n_row * n_col
    me = r * n_col + c
    counts = jnp.sum(acc[...], axis=2)
    parts[c] = counts
    if moved:
        far_counts = jnp.sum(far_acc[...], axis=2)

        @pl.when(inner)
        def _():
            parts[n_col + c] = far_counts

        counts = counts + far_counts
    sums[me] = jnp.sum(counts, axis=0, keepdims=True)

    def send_sum(t, carry):
        dest = lax.rem(me + t, n_all)
        pltpu.make_async_remote_copy(
            src_ref=sums.at[me], dst_ref=sums.at[me],
            send_sem=sum_send.at[0], recv_sem=sum_recv.at[0],
            device_id={"row": dest // n_col, "col": lax.rem(dest, n_col)}, device_id_type=MESH).start()
        return carry

    lax.fori_loop(1, n_all, send_sum, 0)
    out_copies = []
    for t in range(1, n_col):
        out_copies.append(pltpu.make_async_remote_copy(
            src_ref=parts.at[c], dst_ref=parts.at[c],
            send_sem=part_send.at[t - 1], recv_sem=part_recv.at[t - 1],
            device_id={"col": other(c, t, n_col)}, device_id_type=MESH))
    for copy in out_copies:
        copy.start()
    if moved:
        @pl.when(inner)
        def _():
            for t in range(n_col):
                far_part(t).start()
    for copy in sends:
        copy.wait_send()
    for t in range(reach):
        @pl.when((r - t >= 0) & (r < n_row - 1))
        def _():
            col_copy(r - t, 0, r).wait_send()
        @pl.when((r + t < n_row) & (r > 0))
        def _():
            col_copy(r + t, 1, r).wait_send()
    for copy in out_copies:
        copy.wait()
    if moved:
        @pl.when(inner)
        def _():
            for t in range(n_col):
                far_part(t).wait_send()
            parts[n_col] = jnp.zeros(parts.shape[1:], parts.dtype)

        @pl.when(outer)
        def _():
            for t in range(n_col):
                far_part(t).wait_recv()
            parts[n_col] = jnp.sum(parts[n_col:2 * n_col], axis=0)
    plane = jnp.sum(parts[0:n_col], axis=0)
    if moved:
        @pl.when(jnp.logical_not(inner | outer))
        def _():
            parts[n_col] = jnp.zeros(parts.shape[1:], parts.dtype)
        plane = plane + parts[n_col]
    share = width // n_col
    mine = pltpu.roll(plane, lax.rem(width - c * share, width), 1)
    for a in range(rows):
        share_ref[a] = mine[a:a + 1, 0:share] * vertex_scale
    everyone = pltpu.make_async_remote_copy(
        src_ref=sums.at[pl.ds(0, n_all - 1)], dst_ref=sums.at[pl.ds(0, n_all - 1)],
        send_sem=sum_send.at[0], recv_sem=sum_recv.at[0],
        device_id={"col": lax.rem(c + 1, n_col)}, device_id_type=MESH)
    everyone.wait_send()
    everyone.wait_recv()
    total_ref[0, 0] = jnp.sum(sums[...]) * (total_scale / (rows * n_row * width))


def on_device(n_row, n_col, tile_data, tile_cols):
    rows = tile_data.shape[0]
    slots = tile_data.shape[3]
    width = tile_data.shape[4]
    n_tiles = rows * slots
    tiles = tile_data.reshape(n_tiles, width, width)
    cols = jnp.transpose(tile_cols.reshape(rows, slots))
    Y, X = plane_shape(n_col)
    n_far = max(n_col // n_row, 1)
    n_sends = 2 * (n_col + (X - 1) + (Y - 1)) + (X - 1) * (Y - 1) * 2 + (X - 1) + (Y - 1) + 8
    dma = pltpu.SemaphoreType.DMA
    share = width // n_col
    shares, total = pl.pallas_call(
        functools.partial(kernel, n_row, n_col),
        out_shape=(jax.ShapeDtypeStruct((rows, 1, share), jnp.float32),
                   jax.ShapeDtypeStruct((1, 1), jnp.float32)),
        in_specs=[pl.BlockSpec(memory_space=pl.ANY), pl.BlockSpec(memory_space=pl.ANY)],
        out_specs=(pl.BlockSpec(memory_space=pltpu.VMEM), pl.BlockSpec(memory_space=pltpu.SMEM)),
        scratch_shapes=[
            pltpu.VMEM((n_col * n_tiles + 1, width, width), jnp.bfloat16),
            pltpu.VMEM((n_row * n_tiles + 1, width, width), jnp.bfloat16),
            pltpu.VMEM((n_far * n_tiles + 1, width, width), jnp.bfloat16),
            pltpu.VMEM((n_col, slots, rows), jnp.int32),
            pltpu.VMEM((n_row, slots, rows), jnp.int32),
            pltpu.VMEM((n_far, slots, rows), jnp.int32),
            pltpu.SMEM((n_col, slots, rows), jnp.int32),
            pltpu.SMEM((n_row, slots, rows), jnp.int32),
            pltpu.SMEM((n_far, slots, rows), jnp.int32),
            pltpu.VMEM((rows, width, width), jnp.float32),
            pltpu.VMEM((rows, width, width), jnp.float32),
            pltpu.VMEM((2 * n_col, rows, width), jnp.float32),
            pltpu.VMEM((n_row * n_col, 1, width), jnp.float32),
            dma((6,)), dma((3,)),
            dma((n_sends,)), dma((n_col, 2)),
            dma((n_row, 2)), dma((n_row,)),
            dma((n_col + n_row - 2,)), dma((n_col + n_row - 2,)),
            dma((n_col - 1,)), dma((n_col - 1,)),
            dma((1,)), dma((1,)),
            dma((n_far, 2, X + Y)), dma((n_far, 2)),
            dma((n_far, n_col - 1)), dma((n_far,)),
            dma((n_col,)), dma((n_col,)),
        ],
        compiler_params=pltpu.CompilerParams(collective_id=0, has_side_effects=True),
    )(tiles, cols)
    return shares, total[0, 0]


def solution(mesh):
    return jax.shard_map(
        functools.partial(on_device, mesh.shape["row"], mesh.shape["col"]),
        mesh=mesh,
        in_specs=(P(None, "row", "col", None, None, None), P(None, "row", "col", None)),
        out_specs=(P(None, "row", "col"), P()),
        check_vma=False,
    )
```

```python
import functools
import math

import jax
import jax.numpy as jnp
from jax import lax
from jax.experimental import pallas as pl
from jax.experimental.pallas import tpu as pltpu
from jax.sharding import PartitionSpec as P

MESH = pl.DeviceIdType.MESH
vertex_scale = 2.0 ** (-14)
total_scale = 2.0 ** (-12)


def plane_shape(n_col):
    chips = n_col // 2
    side = math.isqrt(chips)
    return (side, side) if side * side == chips else (1, chips)


def kernel(n_row, n_col, tiles, cols_ref, share_ref, total_ref,
           row_buf, col_buf, far_buf, row_idx, col_idx, far_idx, row_smem, col_smem, far_smem,
           acc, far_acc, parts, sums,
           load_sem, smem_sem, row_send, row_recv, col_send, col_recv,
           idx_send, idx_recv, part_send, part_recv, sum_send, sum_recv,
           far_send, far_recv, fidx_send, fidx_recv, fpart_send, fpart_recv):
    r = lax.axis_index("row")
    c = lax.axis_index("col")
    n_tiles = tiles.shape[0]
    half = n_tiles // 2
    rows = acc.shape[0]
    slots = n_tiles // rows
    width = tiles.shape[1]
    zero = n_col * n_tiles
    moved = n_row >= 4 and n_col % n_row == 0
    reach = n_row - 2 if moved else n_row - 1
    n_far = max(n_col // n_row, 1)
    far_zero = n_far * n_tiles
    low = r < n_row // 2
    inner = (r == 1) | (r == n_row - 2)
    outer = (r == 0) | (r == n_row - 1)
    far_left = jnp.where(low, 0, n_row - 1)
    far_middle = n_row - 1 - far_left
    neighbour = jnp.where(low, 1 - r, 2 * n_row - 3 - r)
    Y, X = plane_shape(n_col)
    u = c % 2
    x = (c // 2) % X
    y = c // (2 * X)

    def col_of(yy, xx, uu):
        return (yy * X + xx) * 2 + uu

    def row_block(cc, h):
        return row_buf.at[pl.ds(cc * n_tiles + h * half, half)]

    def col_block(rr):
        return col_buf.at[pl.ds(rr * n_tiles, n_tiles)]

    load_row = pltpu.make_async_copy(tiles, row_buf.at[pl.ds(c * n_tiles, n_tiles)], load_sem.at[0])
    load_row.start()
    load_col = pltpu.make_async_copy(tiles, col_block(r), load_sem.at[1])
    load_col.start()
    load_ri = pltpu.make_async_copy(cols_ref, row_idx.at[c], load_sem.at[2])
    load_ri.start()
    load_ci = pltpu.make_async_copy(cols_ref, col_idx.at[r], load_sem.at[3])
    load_ci.start()

    barrier = pltpu.get_barrier_semaphore()
    for t in range(1, n_col):
        pl.semaphore_signal(barrier, inc=1, device_id={"col": lax.rem(c + t, n_col)}, device_id_type=MESH)
    for t in range(1, n_row):
        pl.semaphore_signal(barrier, inc=1, device_id={"row": lax.rem(r + t, n_row)}, device_id_type=MESH)
    row_buf[zero] = jnp.zeros(row_buf.shape[1:], row_buf.dtype)
    far_buf[far_zero] = jnp.zeros(far_buf.shape[1:], far_buf.dtype)
    col_buf[n_row * n_tiles] = jnp.zeros(col_buf.shape[1:], col_buf.dtype)
    acc[...] = jnp.zeros_like(acc)
    far_acc[...] = jnp.zeros_like(far_acc)
    load_row.wait()
    load_col.wait()
    pl.semaphore_wait(barrier, n_col + n_row - 2)

    sends = []

    def send_row(cc, h, dest):
        copy = pltpu.make_async_remote_copy(
            src_ref=row_block(cc, h), dst_ref=row_block(cc, h),
            send_sem=row_send.at[len(sends)], recv_sem=row_recv.at[cc, h],
            device_id={"col": dest}, device_id_type=MESH)
        copy.start()
        sends.append(copy)

    def got_row(cc, h):
        pltpu.make_async_remote_copy(
            src_ref=row_block(cc, h), dst_ref=row_block(cc, h),
            send_sem=row_send.at[0], recv_sem=row_recv.at[cc, h],
            device_id={"col": lax.rem(c + 1, n_col)}, device_id_type=MESH).wait_recv()

    def col_copy(rr, way, dest):
        return pltpu.make_async_remote_copy(
            src_ref=col_block(rr), dst_ref=col_block(rr),
            send_sem=col_send.at[rr, way], recv_sem=col_recv.at[rr],
            device_id={"row": dest}, device_id_type=MESH)

    def other(value, t, n):
        return lax.rem(value + t, n)

    def pass_on(t):
        up, down = r - t, r + t
        if t > 0:
            @pl.when(up >= 0)
            def _():
                col_copy(up, 0, r).wait_recv()
        if t < reach:
            @pl.when((up >= 0) & (r < n_row - 1))
            def _():
                col_copy(up, 0, r + 1).start()
        if t > 0:
            @pl.when(down < n_row)
            def _():
                col_copy(down, 1, r).wait_recv()
        if t < reach:
            @pl.when((down < n_row) & (r > 0))
            def _():
                col_copy(down, 1, r - 1).start()

    pass_on(0)
    xs = [col_of(y, other(x, t, X), u) for t in range(1, X)]
    ys = [col_of(other(y, t, Y), x, u) for t in range(1, Y)]
    for dest in xs:
        send_row(c, 0, dest)
    for dest in ys:
        send_row(c, 1, dest)
    load_ri.wait()
    load_ci.wait()
    idx_copies = []
    for t in range(1, n_col):
        idx_copies.append(pltpu.make_async_remote_copy(
            src_ref=row_idx.at[c], dst_ref=row_idx.at[c],
            send_sem=idx_send.at[t - 1], recv_sem=idx_recv.at[t - 1],
            device_id={"col": other(c, t, n_col)}, device_id_type=MESH))
    for t in range(1, n_row):
        idx_copies.append(pltpu.make_async_remote_copy(
            src_ref=col_idx.at[r], dst_ref=col_idx.at[r],
            send_sem=idx_send.at[n_col - 2 + t], recv_sem=idx_recv.at[n_col - 2 + t],
            device_id={"row": other(r, t, n_row)}, device_id_type=MESH))
    for copy in idx_copies:
        copy.start()
    for dest in ys:
        send_row(c, 0, dest)
    for dest in xs:
        send_row(c, 1, dest)
    for h in range(2):
        send_row(c, h, c + 1 - 2 * u)
    for t in range(1, max(X, Y)):
        if t < X:
            cc = col_of(y, other(x, t, X), u)
            got_row(cc, 0)
            for dest in ys:
                send_row(cc, 0, dest)
        if t < Y:
            cc = col_of(other(y, t, Y), x, u)
            got_row(cc, 1)
            for dest in xs:
                send_row(cc, 1, dest)
    for t in range(1, X):
        send_row(col_of(y, other(x, t, X), u), 0, c + 1 - 2 * u)
    for t in range(1, Y):
        send_row(col_of(other(y, t, Y), x, u), 1, c + 1 - 2 * u)
    if n_row > 1:
        pass_on(1)

    ways = X + Y

    def far_block(e, h):
        return far_buf.at[pl.ds(e * n_tiles + h * half, half)]

    def far_copy(e, h, way, dest, source=None):
        return pltpu.make_async_remote_copy(
            src_ref=far_block(e, h) if source is None else source, dst_ref=far_block(e, h),
            send_sem=far_send.at[e, h, way], recv_sem=far_recv.at[e, h],
            device_id={"col": dest}, device_id_type=MESH)

    def far_index(e, t):
        return pltpu.make_async_remote_copy(
            src_ref=far_idx.at[e], dst_ref=far_idx.at[e],
            send_sem=fidx_send.at[e, t - 1], recv_sem=fidx_recv.at[e],
            device_id={"col": other(c, t, n_col)}, device_id_type=MESH)

    def far_tiles(e):
        return pltpu.make_async_copy(
            col_buf.at[pl.ds(far_left * n_tiles, n_tiles)],
            far_buf.at[pl.ds(e * n_tiles, n_tiles)], load_sem.at[4])

    def far_place(e):
        cc = e * n_row + far_middle
        return cc, (cc % 2) == u, ((cc // 2) % X) == x, (cc // (2 * X)) == y

    partner = c + 1 - 2 * u
    to_x = [(t, dest) for t, dest in enumerate(xs, 1)]
    to_y = [(X - 1 + t, dest) for t, dest in enumerate(ys, 1)]

    def far_source():
        for e in range(n_far):
            cc, same_u, same_x, same_y = far_place(e)

            @pl.when(inner & (cc == c))
            def _():
                source = col_buf.at[pl.ds(far_left * n_tiles, half)]
                source2 = col_buf.at[pl.ds(far_left * n_tiles + half, half)]
                for way, dest in to_x:
                    far_copy(e, 0, way, dest, source).start()
                for way, dest in to_y:
                    far_copy(e, 1, way, dest, source2).start()
                for way, dest in to_y:
                    far_copy(e, 0, way, dest, source).start()
                for way, dest in to_x:
                    far_copy(e, 1, way, dest, source2).start()
                far_copy(e, 0, 0, partner, source).start()
                far_copy(e, 1, 0, partner, source2).start()
                far_tiles(e).start()
                index = pltpu.make_async_copy(col_idx.at[far_left], far_idx.at[e], load_sem.at[5])
                index.start()
                index.wait()
                for t in range(1, n_col):
                    far_index(e, t).start()

    def far_relay(first):
        for e in range(n_far):
            cc, same_u, same_x, same_y = far_place(e)
            here = inner & same_u & (cc != c)

            @pl.when(here & same_y)
            def _():
                h = 0 if first else 1
                far_copy(e, h, 0, partner).wait_recv()
                if first:
                    for way, dest in to_y:
                        far_copy(e, 0, way, dest).start()
                far_copy(e, h, 0, partner).start()

            @pl.when(here & same_x)
            def _():
                h = 1 if first else 0
                far_copy(e, h, 0, partner).wait_recv()
                if first:
                    for way, dest in to_x:
                        far_copy(e, 1, way, dest).start()
                far_copy(e, h, 0, partner).start()

            if not first:
                @pl.when(here & jnp.logical_not(same_x | same_y))
                def _():
                    for h in range(2):
                        far_copy(e, h, 0, partner).wait_recv()
                        far_copy(e, h, 0, partner).start()

    def far_end():
        for e in range(n_far):
            cc, same_u, same_x, same_y = far_place(e)

            @pl.when(inner & jnp.logical_not(same_u))
            def _():
                for h in range(2):
                    far_copy(e, h, 0, partner).wait_recv()

            @pl.when(inner & (cc == c))
            def _():
                far_tiles(e).wait()
                for t in range(1, n_col):
                    far_index(e, t).wait_send()
                for h in range(2):
                    for way in range(ways - 1):
                        far_copy(e, h, way, partner).wait_send()

            @pl.when(inner & same_u & (cc != c))
            def _():
                for h in range(2):
                    far_copy(e, h, 0, partner).wait_send()

            @pl.when(inner & same_u & (cc != c) & same_y)
            def _():
                for way, dest in to_y:
                    far_copy(e, 0, way, dest).wait_send()

            @pl.when(inner & same_u & (cc != c) & same_x)
            def _():
                for way, dest in to_x:
                    far_copy(e, 1, way, dest).wait_send()

    for copy in idx_copies:
        copy.wait()
    to_smem = [pltpu.make_async_copy(row_idx, row_smem, smem_sem.at[0]),
               pltpu.make_async_copy(col_idx, col_smem, smem_sem.at[1])]
    for copy in to_smem:
        copy.start()
    if moved:
        far_source()
    for t in range(1, X):
        cc = col_of(y, other(x, t, X), u)
        got_row(cc, 1)
        send_row(cc, 1, c + 1 - 2 * u)
    for t in range(1, Y):
        cc = col_of(other(y, t, Y), x, u)
        got_row(cc, 0)
        send_row(cc, 0, c + 1 - 2 * u)
    for tx in range(1, X):
        for ty in range(1, Y):
            cc = col_of(other(y, ty, Y), other(x, tx, X), u)
            for h in range(2):
                got_row(cc, h)
                send_row(cc, h, c + 1 - 2 * u)
    for m in range(n_col // 2):
        for h in range(2):
            got_row(2 * m + 1 - u, h)
    for copy in to_smem:
        copy.wait()

    def unit(rr, left_slot, left_buf, left_zero, own_slot, own_buf, own_zero, own_base, total):
        def step(b, carry):
            middle = b * n_row + rr
            block = lax.rem(middle, n_col)
            left = []
            for a in range(rows):
                index = jnp.int32(left_zero)
                for s in range(slots):
                    held, base = left_slot(block, a, s)
                    index = jnp.where(held == middle, base + a * slots + s, index)
                left.append(left_buf[index])
            right = jnp.concatenate(
                [col_buf[rr * n_tiles + b * slots + s] for s in range(slots)], axis=1)
            own_rows = []
            for a in range(rows):
                pair = []
                for s in range(slots):
                    target = col_smem[rr, s, b]
                    index = jnp.int32(own_zero)
                    for q in range(slots):
                        own = own_slot(a, q)
                        index = jnp.where((own == target) & (target >= 0), own_base + a * slots + q, index)
                    pair.append(own_buf[index])
                own_rows.append(jnp.concatenate(pair, axis=1))
            common = lax.dot_general(
                jnp.concatenate(own_rows, axis=0), right, (((1,), (1,)), ((), ())),
                preferred_element_type=jnp.float32)
            for a in range(rows):
                total[a] += common[a * width:(a + 1) * width] * left[a].astype(jnp.float32)
            return carry
        lax.fori_loop(0, rows, step, 0)

    def near_unit(rr):
        unit(rr, lambda block, a, s: (row_smem[block, s, a], block * n_tiles), row_buf, zero,
             lambda a, q: row_smem[c, q, a], row_buf, zero, c * n_tiles, acc)

    def far_unit():
        unit(far_middle,
             lambda block, a, s: (far_smem[block // n_row, s, a], (block // n_row) * n_tiles),
             far_buf, far_zero,
             lambda a, q: col_smem[far_left, q, a], col_buf, n_row * n_tiles,
             far_left * n_tiles, far_acc)

    def units(t):
        @pl.when(r - t >= 0)
        def _():
            near_unit(r - t)
        @pl.when(r + t < n_row)
        def _():
            near_unit(r + t)

    for t in range(2, reach):
        pass_on(t)
    near_unit(r)
    if moved:
        far_relay(True)
    for t in range(1, reach):
        units(t)
    far_to_smem = pltpu.make_async_copy(far_idx, far_smem, smem_sem.at[2])
    if moved:
        far_relay(False)
        for e in range(n_far):
            @pl.when(inner & (far_place(e)[0] != c))
            def _():
                far_index(e, 1).wait_recv()

        @pl.when(inner)
        def _():
            far_to_smem.start()
    if reach > 1:
        pass_on(reach)
    if reach > 0:
        units(reach)
    if moved:
        far_end()

        @pl.when(inner)
        def _():
            far_to_smem.wait()
            far_unit()

    def far_part(t):
        return pltpu.make_async_remote_copy(
            src_ref=parts.at[n_col + c], dst_ref=parts.at[n_col + c],
            send_sem=fpart_send.at[t], recv_sem=fpart_recv.at[t],
            device_id={"row": neighbour, "col": other(c, t, n_col)}, device_id_type=MESH)

    n_all = n_row * n_col
    me = r * n_col + c
    counts = jnp.sum(acc[...], axis=2)
    parts[c] = counts
    if moved:
        far_counts = jnp.sum(far_acc[...], axis=2)

        @pl.when(inner)
        def _():
            parts[n_col + c] = far_counts

        counts = counts + far_counts
    sums[me] = jnp.sum(counts, axis=0, keepdims=True)

    def send_sum(t, carry):
        dest = lax.rem(me + t, n_all)
        pltpu.make_async_remote_copy(
            src_ref=sums.at[me], dst_ref=sums.at[me],
            send_sem=sum_send.at[0], recv_sem=sum_recv.at[0],
            device_id={"row": dest // n_col, "col": lax.rem(dest, n_col)}, device_id_type=MESH).start()
        return carry

    lax.fori_loop(1, n_all, send_sum, 0)
    out_copies = []
    for t in range(1, n_col):
        out_copies.append(pltpu.make_async_remote_copy(
            src_ref=parts.at[c], dst_ref=parts.at[c],
            send_sem=part_send.at[t - 1], recv_sem=part_recv.at[t - 1],
            device_id={"col": other(c, t, n_col)}, device_id_type=MESH))
    for copy in out_copies:
        copy.start()
    if moved:
        @pl.when(inner)
        def _():
            for t in range(n_col):
                far_part(t).start()
    for copy in sends:
        copy.wait_send()
    for t in range(reach):
        @pl.when((r - t >= 0) & (r < n_row - 1))
        def _():
            col_copy(r - t, 0, r).wait_send()
        @pl.when((r + t < n_row) & (r > 0))
        def _():
            col_copy(r + t, 1, r).wait_send()
    for copy in out_copies:
        copy.wait()
    if moved:
        @pl.when(inner)
        def _():
            for t in range(n_col):
                far_part(t).wait_send()
            parts[n_col] = jnp.zeros(parts.shape[1:], parts.dtype)

        @pl.when(outer)
        def _():
            for t in range(n_col):
                far_part(t).wait_recv()
            parts[n_col] = jnp.sum(parts[n_col:2 * n_col], axis=0)
    plane = jnp.sum(parts[0:n_col], axis=0)
    if moved:
        @pl.when(jnp.logical_not(inner | outer))
        def _():
            parts[n_col] = jnp.zeros(parts.shape[1:], parts.dtype)
        plane = plane + parts[n_col]
    share = width // n_col
    mine = pltpu.roll(plane, lax.rem(width - c * share, width), 1)
    for a in range(rows):
        share_ref[a] = mine[a:a + 1, 0:share] * vertex_scale
    everyone = pltpu.make_async_remote_copy(
        src_ref=sums.at[pl.ds(0, n_all - 1)], dst_ref=sums.at[pl.ds(0, n_all - 1)],
        send_sem=sum_send.at[0], recv_sem=sum_recv.at[0],
        device_id={"col": lax.rem(c + 1, n_col)}, device_id_type=MESH)
    everyone.wait_send()
    everyone.wait_recv()
    total_ref[0, 0] = jnp.sum(sums[...]) * (total_scale / (rows * n_row * width))


def on_device(n_row, n_col, tile_data, tile_cols):
    rows = tile_data.shape[0]
    slots = tile_data.shape[3]
    width = tile_data.shape[4]
    n_tiles = rows * slots
    tiles = tile_data.reshape(n_tiles, width, width)
    cols = jnp.transpose(tile_cols.reshape(rows, slots))
    Y, X = plane_shape(n_col)
    n_far = max(n_col // n_row, 1)
    n_sends = 2 * (n_col + (X - 1) + (Y - 1)) + (X - 1) * (Y - 1) * 2 + (X - 1) + (Y - 1) + 8
    dma = pltpu.SemaphoreType.DMA
    share = width // n_col
    shares, total = pl.pallas_call(
        functools.partial(kernel, n_row, n_col),
        out_shape=(jax.ShapeDtypeStruct((rows, 1, share), jnp.float32),
                   jax.ShapeDtypeStruct((1, 1), jnp.float32)),
        in_specs=[pl.BlockSpec(memory_space=pl.ANY), pl.BlockSpec(memory_space=pl.ANY)],
        out_specs=(pl.BlockSpec(memory_space=pltpu.VMEM), pl.BlockSpec(memory_space=pltpu.SMEM)),
        scratch_shapes=[
            pltpu.VMEM((n_col * n_tiles + 1, width, width), jnp.bfloat16),
            pltpu.VMEM((n_row * n_tiles + 1, width, width), jnp.bfloat16),
            pltpu.VMEM((n_far * n_tiles + 1, width, width), jnp.bfloat16),
            pltpu.VMEM((n_col, slots, rows), jnp.int32),
            pltpu.VMEM((n_row, slots, rows), jnp.int32),
            pltpu.VMEM((n_far, slots, rows), jnp.int32),
            pltpu.SMEM((n_col, slots, rows), jnp.int32),
            pltpu.SMEM((n_row, slots, rows), jnp.int32),
            pltpu.SMEM((n_far, slots, rows), jnp.int32),
            pltpu.VMEM((rows, width, width), jnp.float32),
            pltpu.VMEM((rows, width, width), jnp.float32),
            pltpu.VMEM((2 * n_col, rows, width), jnp.float32),
            pltpu.VMEM((n_row * n_col, 1, width), jnp.float32),
            dma((6,)), dma((3,)),
            dma((n_sends,)), dma((n_col, 2)),
            dma((n_row, 2)), dma((n_row,)),
            dma((n_col + n_row - 2,)), dma((n_col + n_row - 2,)),
            dma((n_col - 1,)), dma((n_col - 1,)),
            dma((1,)), dma((1,)),
            dma((n_far, 2, X + Y)), dma((n_far, 2)),
            dma((n_far, n_col - 1)), dma((n_far,)),
            dma((n_col,)), dma((n_col,)),
        ],
        compiler_params=pltpu.CompilerParams(collective_id=0, has_side_effects=True),
    )(tiles, cols)
    return shares, total[0, 0]


def solution(mesh):
    return jax.shard_map(
        functools.partial(on_device, mesh.shape["row"], mesh.shape["col"]),
        mesh=mesh,
        in_specs=(P(None, "row", "col", None, None, None), P(None, "row", "col", None)),
        out_specs=(P(None, "row", "col"), P()),
        check_vma=False,
    )
```

```python
import functools
import math

import jax
import jax.numpy as jnp
from jax import lax
from jax.experimental import pallas as pl
from jax.experimental.pallas import tpu as pltpu
from jax.sharding import PartitionSpec as P

MESH = pl.DeviceIdType.MESH
vertex_scale = 2.0 ** (-14)
total_scale = 2.0 ** (-12)


def plane_shape(n_col):
    chips = n_col // 2
    side = math.isqrt(chips)
    return (side, side) if side * side == chips else (1, chips)


def kernel(n_row, n_col, tiles, cols_ref, share_ref, total_ref,
           row_buf, col_buf, far_buf, row_idx, col_idx, far_idx, row_smem, col_smem, far_smem,
           acc, far_acc, parts, sums,
           load_sem, smem_sem, row_send, row_recv, col_send, col_recv,
           idx_send, idx_recv, part_send, part_recv, sum_send, sum_recv,
           far_send, far_recv, fidx_send, fidx_recv, fpart_send, fpart_recv):
    r = lax.axis_index("row")
    c = lax.axis_index("col")
    n_tiles = tiles.shape[0]
    half = n_tiles // 2
    rows = acc.shape[0]
    slots = n_tiles // rows
    width = tiles.shape[1]
    zero = n_col * n_tiles
    moved = n_row >= 4 and n_col % n_row == 0
    reach = n_row - 2 if moved else n_row - 1
    n_far = max(n_col // n_row, 1)
    far_zero = n_far * n_tiles
    low = r < n_row // 2
    inner = (r == 1) | (r == n_row - 2)
    outer = (r == 0) | (r == n_row - 1)
    far_left = jnp.where(low, 0, n_row - 1)
    far_middle = n_row - 1 - far_left
    neighbour = jnp.where(low, 1 - r, 2 * n_row - 3 - r)
    Y, X = plane_shape(n_col)
    u = c % 2
    x = (c // 2) % X
    y = c // (2 * X)

    def col_of(yy, xx, uu):
        return (yy * X + xx) * 2 + uu

    def row_block(cc, h):
        return row_buf.at[pl.ds(cc * n_tiles + h * half, half)]

    def col_block(rr):
        return col_buf.at[pl.ds(rr * n_tiles, n_tiles)]

    load_row = pltpu.make_async_copy(tiles, row_buf.at[pl.ds(c * n_tiles, n_tiles)], load_sem.at[0])
    load_row.start()
    load_col = pltpu.make_async_copy(tiles, col_block(r), load_sem.at[1])
    load_col.start()
    load_ri = pltpu.make_async_copy(cols_ref, row_idx.at[c], load_sem.at[2])
    load_ri.start()
    load_ci = pltpu.make_async_copy(cols_ref, col_idx.at[r], load_sem.at[3])
    load_ci.start()

    barrier = pltpu.get_barrier_semaphore()
    for t in range(1, n_col):
        pl.semaphore_signal(barrier, inc=1, device_id={"col": lax.rem(c + t, n_col)}, device_id_type=MESH)
    for t in range(1, n_row):
        pl.semaphore_signal(barrier, inc=1, device_id={"row": lax.rem(r + t, n_row)}, device_id_type=MESH)
    row_buf[zero] = jnp.zeros(row_buf.shape[1:], row_buf.dtype)
    far_buf[far_zero] = jnp.zeros(far_buf.shape[1:], far_buf.dtype)
    col_buf[n_row * n_tiles] = jnp.zeros(col_buf.shape[1:], col_buf.dtype)
    acc[...] = jnp.zeros_like(acc)
    far_acc[...] = jnp.zeros_like(far_acc)
    load_row.wait()
    load_col.wait()
    pl.semaphore_wait(barrier, n_col + n_row - 2)

    sends = []

    def send_row(cc, h, dest):
        copy = pltpu.make_async_remote_copy(
            src_ref=row_block(cc, h), dst_ref=row_block(cc, h),
            send_sem=row_send.at[len(sends)], recv_sem=row_recv.at[cc, h],
            device_id={"col": dest}, device_id_type=MESH)
        copy.start()
        sends.append(copy)

    def got_row(cc, h):
        pltpu.make_async_remote_copy(
            src_ref=row_block(cc, h), dst_ref=row_block(cc, h),
            send_sem=row_send.at[0], recv_sem=row_recv.at[cc, h],
            device_id={"col": lax.rem(c + 1, n_col)}, device_id_type=MESH).wait_recv()

    def col_copy(rr, way, dest):
        return pltpu.make_async_remote_copy(
            src_ref=col_block(rr), dst_ref=col_block(rr),
            send_sem=col_send.at[rr, way], recv_sem=col_recv.at[rr],
            device_id={"row": dest}, device_id_type=MESH)

    def other(value, t, n):
        return lax.rem(value + t, n)

    def pass_on(t):
        up, down = r - t, r + t
        if t > 0:
            @pl.when(up >= 0)
            def _():
                col_copy(up, 0, r).wait_recv()
        if t < reach:
            @pl.when((up >= 0) & (r < n_row - 1))
            def _():
                col_copy(up, 0, r + 1).start()
        if t > 0:
            @pl.when(down < n_row)
            def _():
                col_copy(down, 1, r).wait_recv()
        if t < reach:
            @pl.when((down < n_row) & (r > 0))
            def _():
                col_copy(down, 1, r - 1).start()

    pass_on(0)
    xs = [col_of(y, other(x, t, X), u) for t in range(1, X)]
    ys = [col_of(other(y, t, Y), x, u) for t in range(1, Y)]
    for dest in xs:
        send_row(c, 0, dest)
    for dest in ys:
        send_row(c, 1, dest)
    load_ri.wait()
    load_ci.wait()
    idx_copies = []
    for t in range(1, n_col):
        idx_copies.append(pltpu.make_async_remote_copy(
            src_ref=row_idx.at[c], dst_ref=row_idx.at[c],
            send_sem=idx_send.at[t - 1], recv_sem=idx_recv.at[t - 1],
            device_id={"col": other(c, t, n_col)}, device_id_type=MESH))
    for t in range(1, n_row):
        idx_copies.append(pltpu.make_async_remote_copy(
            src_ref=col_idx.at[r], dst_ref=col_idx.at[r],
            send_sem=idx_send.at[n_col - 2 + t], recv_sem=idx_recv.at[n_col - 2 + t],
            device_id={"row": other(r, t, n_row)}, device_id_type=MESH))
    for copy in idx_copies:
        copy.start()
    for dest in ys:
        send_row(c, 0, dest)
    for dest in xs:
        send_row(c, 1, dest)
    for h in range(2):
        send_row(c, h, c + 1 - 2 * u)
    for t in range(1, max(X, Y)):
        if t < X:
            cc = col_of(y, other(x, t, X), u)
            got_row(cc, 0)
            for dest in ys:
                send_row(cc, 0, dest)
        if t < Y:
            cc = col_of(other(y, t, Y), x, u)
            got_row(cc, 1)
            for dest in xs:
                send_row(cc, 1, dest)
    for t in range(1, X):
        send_row(col_of(y, other(x, t, X), u), 0, c + 1 - 2 * u)
    for t in range(1, Y):
        send_row(col_of(other(y, t, Y), x, u), 1, c + 1 - 2 * u)
    if n_row > 1:
        pass_on(1)

    ways = X + Y

    def far_block(e, h):
        return far_buf.at[pl.ds(e * n_tiles + h * half, half)]

    def far_copy(e, h, way, dest, source=None):
        return pltpu.make_async_remote_copy(
            src_ref=far_block(e, h) if source is None else source, dst_ref=far_block(e, h),
            send_sem=far_send.at[e, h, way], recv_sem=far_recv.at[e, h],
            device_id={"col": dest}, device_id_type=MESH)

    def far_index(e, t):
        return pltpu.make_async_remote_copy(
            src_ref=far_idx.at[e], dst_ref=far_idx.at[e],
            send_sem=fidx_send.at[e, t - 1], recv_sem=fidx_recv.at[e],
            device_id={"col": other(c, t, n_col)}, device_id_type=MESH)

    def far_tiles(e):
        return pltpu.make_async_copy(
            col_buf.at[pl.ds(far_left * n_tiles, n_tiles)],
            far_buf.at[pl.ds(e * n_tiles, n_tiles)], load_sem.at[4])

    def far_place(e):
        cc = e * n_row + far_middle
        return cc, (cc % 2) == u, ((cc // 2) % X) == x, (cc // (2 * X)) == y

    partner = c + 1 - 2 * u
    to_x = [(t, dest) for t, dest in enumerate(xs, 1)]
    to_y = [(X - 1 + t, dest) for t, dest in enumerate(ys, 1)]

    def far_source():
        for e in range(n_far):
            cc, same_u, same_x, same_y = far_place(e)

            @pl.when(inner & (cc == c))
            def _():
                source = col_buf.at[pl.ds(far_left * n_tiles, half)]
                source2 = col_buf.at[pl.ds(far_left * n_tiles + half, half)]
                for way, dest in to_x:
                    far_copy(e, 0, way, dest, source).start()
                for way, dest in to_y:
                    far_copy(e, 1, way, dest, source2).start()
                for way, dest in to_y:
                    far_copy(e, 0, way, dest, source).start()
                for way, dest in to_x:
                    far_copy(e, 1, way, dest, source2).start()
                far_copy(e, 0, 0, partner, source).start()
                far_copy(e, 1, 0, partner, source2).start()
                far_tiles(e).start()
                index = pltpu.make_async_copy(col_idx.at[far_left], far_idx.at[e], load_sem.at[5])
                index.start()
                index.wait()
                for t in range(1, n_col):
                    far_index(e, t).start()

    def far_relay(first):
        for e in range(n_far):
            cc, same_u, same_x, same_y = far_place(e)
            here = inner & same_u & (cc != c)

            @pl.when(here & same_y)
            def _():
                h = 0 if first else 1
                far_copy(e, h, 0, partner).wait_recv()
                if first:
                    for way, dest in to_y:
                        far_copy(e, 0, way, dest).start()
                far_copy(e, h, 0, partner).start()

            @pl.when(here & same_x)
            def _():
                h = 1 if first else 0
                far_copy(e, h, 0, partner).wait_recv()
                if first:
                    for way, dest in to_x:
                        far_copy(e, 1, way, dest).start()
                far_copy(e, h, 0, partner).start()

            if not first:
                @pl.when(here & jnp.logical_not(same_x | same_y))
                def _():
                    for h in range(2):
                        far_copy(e, h, 0, partner).wait_recv()
                        far_copy(e, h, 0, partner).start()

    def far_end():
        for e in range(n_far):
            cc, same_u, same_x, same_y = far_place(e)

            @pl.when(inner & jnp.logical_not(same_u))
            def _():
                for h in range(2):
                    far_copy(e, h, 0, partner).wait_recv()

            @pl.when(inner & (cc == c))
            def _():
                far_tiles(e).wait()
                for t in range(1, n_col):
                    far_index(e, t).wait_send()
                for h in range(2):
                    for way in range(ways - 1):
                        far_copy(e, h, way, partner).wait_send()

            @pl.when(inner & same_u & (cc != c))
            def _():
                for h in range(2):
                    far_copy(e, h, 0, partner).wait_send()

            @pl.when(inner & same_u & (cc != c) & same_y)
            def _():
                for way, dest in to_y:
                    far_copy(e, 0, way, dest).wait_send()

            @pl.when(inner & same_u & (cc != c) & same_x)
            def _():
                for way, dest in to_x:
                    far_copy(e, 1, way, dest).wait_send()

    for copy in idx_copies:
        copy.wait()
    to_smem = [pltpu.make_async_copy(row_idx, row_smem, smem_sem.at[0]),
               pltpu.make_async_copy(col_idx, col_smem, smem_sem.at[1])]
    for copy in to_smem:
        copy.start()
    if moved:
        far_source()
    for t in range(1, X):
        cc = col_of(y, other(x, t, X), u)
        got_row(cc, 1)
        send_row(cc, 1, c + 1 - 2 * u)
    for t in range(1, Y):
        cc = col_of(other(y, t, Y), x, u)
        got_row(cc, 0)
        send_row(cc, 0, c + 1 - 2 * u)
    for tx in range(1, X):
        for ty in range(1, Y):
            cc = col_of(other(y, ty, Y), other(x, tx, X), u)
            for h in range(2):
                got_row(cc, h)
                send_row(cc, h, c + 1 - 2 * u)
    for m in range(n_col // 2):
        for h in range(2):
            got_row(2 * m + 1 - u, h)
    for copy in to_smem:
        copy.wait()

    def unit(rr, left_slot, left_buf, left_zero, own_slot, own_buf, own_zero, own_base, total):
        def step(b, carry):
            middle = b * n_row + rr
            block = lax.rem(middle, n_col)
            left = []
            for a in range(rows):
                index = jnp.int32(left_zero)
                for s in range(slots):
                    held, base = left_slot(block, a, s)
                    index = jnp.where(held == middle, base + a * slots + s, index)
                left.append(left_buf[index])
            right = jnp.concatenate(
                [col_buf[rr * n_tiles + b * slots + s] for s in range(slots)], axis=1)
            own_rows = []
            for a in range(rows):
                pair = []
                for s in range(slots):
                    target = col_smem[rr, s, b]
                    index = jnp.int32(own_zero)
                    for q in range(slots):
                        own = own_slot(a, q)
                        index = jnp.where((own == target) & (target >= 0), own_base + a * slots + q, index)
                    pair.append(own_buf[index])
                own_rows.append(jnp.concatenate(pair, axis=1))
            common = lax.dot_general(
                jnp.concatenate(own_rows, axis=0), right, (((1,), (1,)), ((), ())),
                preferred_element_type=jnp.float32)
            for a in range(rows):
                total[a] += common[a * width:(a + 1) * width] * left[a].astype(jnp.float32)
            return carry
        lax.fori_loop(0, rows, step, 0)

    def near_unit(rr):
        unit(rr, lambda block, a, s: (row_smem[block, s, a], block * n_tiles), row_buf, zero,
             lambda a, q: row_smem[c, q, a], row_buf, zero, c * n_tiles, acc)

    def far_unit():
        unit(far_middle,
             lambda block, a, s: (far_smem[block // n_row, s, a], (block // n_row) * n_tiles),
             far_buf, far_zero,
             lambda a, q: col_smem[far_left, q, a], col_buf, n_row * n_tiles,
             far_left * n_tiles, far_acc)

    def units(t):
        @pl.when(r - t >= 0)
        def _():
            near_unit(r - t)
        @pl.when(r + t < n_row)
        def _():
            near_unit(r + t)

    for t in range(2, reach):
        pass_on(t)
    near_unit(r)
    if moved:
        far_relay(True)
    for t in range(1, reach):
        units(t)
    if reach > 1:
        pass_on(reach)
    if reach > 0:
        units(reach)
    far_to_smem = pltpu.make_async_copy(far_idx, far_smem, smem_sem.at[2])
    if moved:
        far_relay(False)
        for e in range(n_far):
            @pl.when(inner & (far_place(e)[0] != c))
            def _():
                far_index(e, 1).wait_recv()

        @pl.when(inner)
        def _():
            far_to_smem.start()
    if moved:
        far_end()

        @pl.when(inner)
        def _():
            far_to_smem.wait()
            far_unit()

    def far_part(t):
        return pltpu.make_async_remote_copy(
            src_ref=parts.at[n_col + c], dst_ref=parts.at[n_col + c],
            send_sem=fpart_send.at[t], recv_sem=fpart_recv.at[t],
            device_id={"row": neighbour, "col": other(c, t, n_col)}, device_id_type=MESH)

    n_all = n_row * n_col
    me = r * n_col + c
    counts = jnp.sum(acc[...], axis=2)
    parts[c] = counts
    if moved:
        far_counts = jnp.sum(far_acc[...], axis=2)

        @pl.when(inner)
        def _():
            parts[n_col + c] = far_counts

        counts = counts + far_counts
    sums[me] = jnp.sum(counts, axis=0, keepdims=True)

    def send_sum(t, carry):
        dest = lax.rem(me + t, n_all)
        pltpu.make_async_remote_copy(
            src_ref=sums.at[me], dst_ref=sums.at[me],
            send_sem=sum_send.at[0], recv_sem=sum_recv.at[0],
            device_id={"row": dest // n_col, "col": lax.rem(dest, n_col)}, device_id_type=MESH).start()
        return carry

    lax.fori_loop(1, n_all, send_sum, 0)
    out_copies = []
    for t in range(1, n_col):
        out_copies.append(pltpu.make_async_remote_copy(
            src_ref=parts.at[c], dst_ref=parts.at[c],
            send_sem=part_send.at[t - 1], recv_sem=part_recv.at[t - 1],
            device_id={"col": other(c, t, n_col)}, device_id_type=MESH))
    for copy in out_copies:
        copy.start()
    if moved:
        @pl.when(inner)
        def _():
            for t in range(n_col):
                far_part(t).start()
    for copy in sends:
        copy.wait_send()
    for t in range(reach):
        @pl.when((r - t >= 0) & (r < n_row - 1))
        def _():
            col_copy(r - t, 0, r).wait_send()
        @pl.when((r + t < n_row) & (r > 0))
        def _():
            col_copy(r + t, 1, r).wait_send()
    for copy in out_copies:
        copy.wait()
    if moved:
        @pl.when(inner)
        def _():
            for t in range(n_col):
                far_part(t).wait_send()
            parts[n_col] = jnp.zeros(parts.shape[1:], parts.dtype)

        @pl.when(outer)
        def _():
            for t in range(n_col):
                far_part(t).wait_recv()
            parts[n_col] = jnp.sum(parts[n_col:2 * n_col], axis=0)
    plane = jnp.sum(parts[0:n_col], axis=0)
    if moved:
        @pl.when(jnp.logical_not(inner | outer))
        def _():
            parts[n_col] = jnp.zeros(parts.shape[1:], parts.dtype)
        plane = plane + parts[n_col]
    share = width // n_col
    mine = pltpu.roll(plane, lax.rem(width - c * share, width), 1)
    for a in range(rows):
        share_ref[a] = mine[a:a + 1, 0:share] * vertex_scale
    everyone = pltpu.make_async_remote_copy(
        src_ref=sums.at[pl.ds(0, n_all - 1)], dst_ref=sums.at[pl.ds(0, n_all - 1)],
        send_sem=sum_send.at[0], recv_sem=sum_recv.at[0],
        device_id={"col": lax.rem(c + 1, n_col)}, device_id_type=MESH)
    everyone.wait_send()
    everyone.wait_recv()
    total_ref[0, 0] = jnp.sum(sums[...]) * (total_scale / (rows * n_row * width))


def on_device(n_row, n_col, tile_data, tile_cols):
    rows = tile_data.shape[0]
    slots = tile_data.shape[3]
    width = tile_data.shape[4]
    n_tiles = rows * slots
    tiles = tile_data.reshape(n_tiles, width, width)
    cols = jnp.transpose(tile_cols.reshape(rows, slots))
    Y, X = plane_shape(n_col)
    n_far = max(n_col // n_row, 1)
    n_sends = 2 * (n_col + (X - 1) + (Y - 1)) + (X - 1) * (Y - 1) * 2 + (X - 1) + (Y - 1) + 8
    dma = pltpu.SemaphoreType.DMA
    share = width // n_col
    shares, total = pl.pallas_call(
        functools.partial(kernel, n_row, n_col),
        out_shape=(jax.ShapeDtypeStruct((rows, 1, share), jnp.float32),
                   jax.ShapeDtypeStruct((1, 1), jnp.float32)),
        in_specs=[pl.BlockSpec(memory_space=pl.ANY), pl.BlockSpec(memory_space=pl.ANY)],
        out_specs=(pl.BlockSpec(memory_space=pltpu.VMEM), pl.BlockSpec(memory_space=pltpu.SMEM)),
        scratch_shapes=[
            pltpu.VMEM((n_col * n_tiles + 1, width, width), jnp.bfloat16),
            pltpu.VMEM((n_row * n_tiles + 1, width, width), jnp.bfloat16),
            pltpu.VMEM((n_far * n_tiles + 1, width, width), jnp.bfloat16),
            pltpu.VMEM((n_col, slots, rows), jnp.int32),
            pltpu.VMEM((n_row, slots, rows), jnp.int32),
            pltpu.VMEM((n_far, slots, rows), jnp.int32),
            pltpu.SMEM((n_col, slots, rows), jnp.int32),
            pltpu.SMEM((n_row, slots, rows), jnp.int32),
            pltpu.SMEM((n_far, slots, rows), jnp.int32),
            pltpu.VMEM((rows, width, width), jnp.float32),
            pltpu.VMEM((rows, width, width), jnp.float32),
            pltpu.VMEM((2 * n_col, rows, width), jnp.float32),
            pltpu.VMEM((n_row * n_col, 1, width), jnp.float32),
            dma((6,)), dma((3,)),
            dma((n_sends,)), dma((n_col, 2)),
            dma((n_row, 2)), dma((n_row,)),
            dma((n_col + n_row - 2,)), dma((n_col + n_row - 2,)),
            dma((n_col - 1,)), dma((n_col - 1,)),
            dma((1,)), dma((1,)),
            dma((n_far, 2, X + Y)), dma((n_far, 2)),
            dma((n_far, n_col - 1)), dma((n_far,)),
            dma((n_col,)), dma((n_col,)),
        ],
        compiler_params=pltpu.CompilerParams(collective_id=0, has_side_effects=True),
    )(tiles, cols)
    return shares, total[0, 0]


def solution(mesh):
    return jax.shard_map(
        functools.partial(on_device, mesh.shape["row"], mesh.shape["col"]),
        mesh=mesh,
        in_specs=(P(None, "row", "col", None, None, None), P(None, "row", "col", None)),
        out_specs=(P(None, "row", "col"), P()),
        check_vma=False,
    )
```
